32 devices in a mesh: member: 2 (over x), tensor: 4 (over y, core), answer: 4 (over z).
Axes of the slice: x: 2, y: 2, z: 4, core: 2. Of those that a mesh axis runs over, the one named last changes fastest.
Arguments:
- master: float32 [5120, 13824], P('member', ('tensor', 'answer')), may hold values from -6 to 6
- left_noise: bfloat16 [256, 5120], P(('member', 'answer')), may hold values from -5 to 5
- right_noise: bfloat16 [256, 13824], P(('member', 'answer'), 'tensor'), may hold values from -5 to 5
- returns: float32 [256, 512], P('member', 'answer'), may hold values from -12 to 12
Outputs:
- new_master: float32 [5120, 13824], P('member', ('tensor', 'answer'))
- rollout: bfloat16 [5120, 13824], P(('member', 'answer'), 'tensor')
The draws below stay inside these ranges and needn't reach their ends.
All inputs are finite; a program needn't handle non-finite values.
Results may differ from the reference program's by a relative error of at most 0.01.
Values may be sent and summed in bfloat16 or wider, within the bound.
A program may use at most 64 MiB of HBM per device.

```python
import jax
import jax.numpy as jnp
from jax import lax

DMODEL = 5120
DFF = 13824
POP = 256
ANSWERS = 512


def draw_returns(key, part):
    position = jnp.arange(POP, dtype=jnp.float32) / max(POP - 1, 1)
    rising = 1.0 + 2.0 * position
    base = jax.random.normal(key, (POP, ANSWERS), jnp.float32)
    offset = 0.1
    return jnp.clip((base + offset) * rising[:, None], -12.0, 12.0)


def level_of(rng, shape, cuts, least, high):
    level, own = 1.0, jax.random.fold_in(rng, 6)
    for dim, blocks in cuts:
        draws = jnp.exp(jax.random.uniform(jax.random.fold_in(own, dim), (blocks,), jnp.float32, least / len(cuts), high / len(cuts)))
        level = level * jnp.repeat(draws, shape[dim] // blocks).reshape([-1 if axis == dim else 1 for axis in range(len(shape))])
    return level


def centred(own_key, shape, spread, bound, shards=(), kind=jnp.bfloat16):
    array = spread * jax.random.normal(own_key, shape, jnp.float32)
    if shards:
        array = array * level_of(own_key, shape, shards, -0.22, 0.18)
    return jnp.clip(array, -bound, bound).astype(kind)


def setup_inputs(seed: int = 0) -> dict:
    splits = jax.random.split(jax.random.key(seed), 5)
    return {
        "master": centred(splits[0], (DMODEL, DFF), 1.0, 6.0, ((0, 2), (1, 16)), jnp.float32),
        "left_noise": centred(splits[1], (POP, DMODEL), 1.0, 5.0, ((0, 8),)),
        "right_noise": centred(splits[2], (POP, DFF), 1.0, 5.0, ((0, 8), (1, 4))),
        "returns": draw_returns(jax.random.fold_in(splits[4], 71), 0),
    }


def reference(master, left_noise, right_noise, returns):
    scores = lax.optimization_barrier(jnp.sum(returns, axis=1))
    population = scores.shape[0]
    average = jnp.sum(scores) / population
    variance = jnp.sum(scores * scores) / population - average * average
    fitness = (scores - average) / jnp.sqrt(variance + 1e-05)
    weighted = left_noise.astype(jnp.float32) * fitness[:, None]
    update = lax.dot_general(weighted, right_noise.astype(jnp.float32), (((0,), (0,)), ((), ())), precision=lax.Precision.HIGHEST)
    new_master = master + update / jnp.sqrt(jnp.float32(population))
    return (new_master, new_master.astype(jnp.bfloat16))
```

```python
import jax
import jax.numpy as jnp
from jax import lax
from jax.experimental import pallas as pl
from jax.experimental.pallas import tpu as pltpu
from jax.sharding import PartitionSpec as P


def contract(left_tile, accum, pieces):
    right_cols, weights = pieces
    weighted = left_tile.astype(jnp.float32) * weights[:, None]
    return accum + lax.dot_general(
        weighted,
        right_cols.astype(jnp.float32),
        (((0,), (0,)), ((), ())),
        precision=lax.Precision.HIGHEST,
    )


def plain_body(master, left_noise, right_noise, returns):
    member_count = lax.axis_size("member")
    answer_count = lax.axis_size("answer")
    partial_value = jnp.sum(returns, axis=1)
    block_len = partial_value.shape[0]
    population = block_len * member_count
    scores = lax.psum(partial_value, "answer")
    score_sum, square_sum = lax.psum((jnp.sum(scores), jnp.sum(scores * scores)), "member")
    average = score_sum / population
    variance = square_sum / population - average * average
    fitness = (scores - average) / jnp.sqrt(variance + 1e-05)
    tile_rows = master.shape[0]
    local_members = left_noise.shape[0]
    restricted = lax.all_to_all(left_noise, "member", split_axis=1, concat_axis=0, tiled=True)
    gathered_rows = lax.all_gather(restricted, "answer", axis=0, tiled=True)
    width = gathered_rows.shape[1]
    left_tile = gathered_rows.reshape(answer_count, member_count, local_members, width)
    left_tile = jnp.transpose(left_tile, (1, 0, 2, 3)).reshape(
        answer_count * member_count * local_members, width
    )
    right_block = lax.all_to_all(right_noise, "answer", split_axis=1, concat_axis=0, tiled=True)
    initial = jnp.zeros((tile_rows, right_block.shape[1]), jnp.float32)
    update = contract(
        left_tile,
        initial,
        (
            lax.all_gather(right_block, "member", axis=0, tiled=True),
            lax.all_gather(fitness.astype(jnp.bfloat16), "member", axis=0, tiled=True).astype(
                jnp.float32
            ),
        ),
    )
    new_master = master + update / jnp.sqrt(jnp.float32(population))
    rollout = lax.all_to_all(
        new_master.astype(jnp.bfloat16), "answer", split_axis=0, concat_axis=1, tiled=True
    )
    return (new_master, rollout)


def exchange_kernel(members, chunks, left_ref, right_ref, returns_ref, master_ref, *refs):
    sides = 3
    l_ref, r_ref, s_ref, p_ref, e_ref, *refs = refs
    blocks, refs = refs[:sides * len(chunks)], refs[sides * len(chunks):]
    (wide, narrow, part, own_sem, pull_sem, push_sem, s_send, s_recv, x_send, x_recv, f_send, f_recv,
     z_send, z_recv, q_send, q_recv, y_send, y_recv, e_send, e_recv) = refs
    me, te, an = lax.axis_index("member"), lax.axis_index("tensor"), lax.axis_index("answer")
    answers = 4
    local = left_ref.shape[0]
    slab = local * members
    tile = l_ref.shape[1]
    piece = tile // 4
    rows = tile // answers
    beside = lambda i: i + 1 - 2 * lax.rem(i, 2)
    other, core, across = 1 - me, beside(te), lax.rem(te + 2, 4)
    near, far = beside(an), 2 - lax.div(an, 2)
    beyond = 2 * (1 - lax.div(an, 2))
    inner = lax.div(an + 1, 2) == 1
    pair = {1: near, 2: lax.rem(an + 2, answers), 3: answers - 1 - an}

    def l_at(start, count, t):
        return l_ref.at[pl.ds(pl.multiple_of(start, local), count), pl.ds(pl.multiple_of(t * piece, piece), piece)]

    def l_slab(a, t):
        return l_at(a * slab, slab, t)

    def r_at(a, m):
        return r_ref.at[pl.ds(pl.multiple_of((a * members + m) * local, local), local), :]

    def remote(src, dst, send, recv, where):
        return pltpu.make_async_remote_copy(src_ref=src, dst_ref=dst, send_sem=send, recv_sem=recv,
                                            device_id=where, device_id_type=pl.DeviceIdType.MESH)

    def pull(x):
        return pltpu.make_async_copy(
            master_ref.at[:, pl.ds(pl.multiple_of(pair[x] * rows, rows), rows)], wide.at[x % 2], pull_sem.at[x - 1])

    def push(x, c):
        at = sum(chunks[:c])
        return pltpu.make_async_copy(
            narrow.at[x % 2, :, at:at + chunks[c]], blocks[(x - 1) * len(chunks) + c], push_sem.at[x - 1, c])

    def cast(x):
        pull(x).wait()
        step = 96

        def one(i, _):
            at = pl.ds(pl.multiple_of(i * step, step), step)
            narrow[x % 2, at, :] = wide[x % 2, at, :].astype(narrow.dtype)
            return 0

        lax.fori_loop(0, narrow.shape[1] // step, one, 0)
        for c in range(len(chunks)):
            push(x, c).start()

    pull(3).start()
    pull(2).start()
    own_l = pltpu.make_async_copy(
        left_ref.at[:, pl.ds(pl.multiple_of(me * tile + te * piece, piece), piece)],
        l_at((an * members + me) * local, local, te), own_sem.at[0])
    own_r = pltpu.make_async_copy(right_ref, r_at(an, me), own_sem.at[1])
    own_l.start()
    own_r.start()
    part[...] = jnp.sum(returns_ref[...].T, axis=0, keepdims=True)
    own_p = pltpu.make_async_copy(part, p_ref, own_sem.at[2])
    own_s = pltpu.make_async_copy(part, s_ref.at[an * members + me], own_sem.at[3])
    own_p.start()
    own_s.start()

    barrier = pltpu.get_barrier_semaphore()
    peers = [(dm, da) for dm in range(members) for da in range(answers) if (dm, da) != (0, 0)]
    place = lambda dm, da: {"member": lax.rem(me + dm, members), "answer": lax.rem(an + da, answers)}
    for dm, da in peers:
        pl.semaphore_signal(barrier, inc=1, device_id=place(dm, da), device_id_type=pl.DeviceIdType.MESH)
    for t in (core, across):
        pl.semaphore_signal(barrier, inc=1, device_id={"tensor": t}, device_id_type=pl.DeviceIdType.MESH)
    pl.semaphore_wait(barrier, len(peers) + 2)

    mine = lax.rem(an, 2)
    r_near = remote(right_ref, r_at(an, me), z_send.at[0], z_recv.at[0], {"answer": near})
    r_far = remote(right_ref, r_at(an, me), z_send.at[1], z_recv.at[1 + mine], {"answer": far})
    l_over = remote(left_ref.at[:, pl.ds(pl.multiple_of(other * tile + te * piece, piece), piece)],
                    l_at((an * members + me) * local, local, te), x_send.at[0], x_recv.at[0], {"member": other})
    forward = {0: remote(right_ref, r_at(an, me), f_send.at[0], f_recv.at[0], {"member": other})}
    l_over.start()
    r_far.start()
    r_near.start()
    forward[0].start()
    own_p.wait()
    scores = []
    for i, (dm, da) in enumerate(peers):
        copy = remote(p_ref, s_ref.at[an * members + me], s_send.at[i], s_recv.at[i], place(dm, da))
        copy.start()
        scores.append(copy)
    own_l.wait()
    l_over.wait_recv()
    l_near = remote(l_slab(an, te), l_slab(an, te), q_send.at[0], q_recv.at[0], {"answer": near})
    l_far = remote(l_slab(an, te), l_slab(an, te), q_send.at[1], q_recv.at[1 + mine], {"answer": far})
    l_far.start()
    l_near.start()
    cast(3)
    push(3, 0).wait()
    early = remote(blocks[2 * len(chunks)], e_ref, e_send, e_recv, {"answer": pair[3]})
    early.start()
    for c in range(1, len(chunks)):
        push(3, c).wait()
    pull(1).start()
    cast(2)
    cast(1)

    sources = (near, beyond, beyond + 1)
    r_relays, l_relays = {}, {}
    for k, source in enumerate(sources):
        block = r_at(source, me)
        remote(block, block, z_send.at[0], z_recv.at[k], {"answer": near}).wait_recv()
        forward[k + 1] = remote(block, block, f_send.at[k + 1], f_recv.at[k + 1], {"member": other})
        forward[k + 1].start()
        if k:
            r_relays[k] = remote(block, block, z_send.at[1 + k], z_recv.at[k], {"answer": near})
            pl.when(inner)(r_relays[k].start)
        block = l_slab(source, te)
        remote(block, block, q_send.at[0], q_recv.at[k], {"answer": near}).wait_recv()
        if k:
            l_relays[k] = remote(block, block, q_send.at[1 + k], q_recv.at[k], {"answer": near})
            pl.when(inner)(l_relays[k].start)
    total = slab * answers
    l_y = remote(l_at(0, total, te), l_at(0, total, te), y_send.at[0], y_recv.at[0], {"tensor": across})
    l_c = remote(l_at(0, total, te), l_at(0, total, te), y_send.at[1], y_recv.at[1], {"tensor": core})
    l_y.start()
    l_c.start()
    block = l_at(0, total, across)
    remote(block, block, y_send.at[0], y_recv.at[0], {"tensor": across}).wait_recv()
    l_d = remote(block, block, y_send.at[2], y_recv.at[2], {"tensor": core})
    l_d.start()
    for i, (dm, da) in enumerate(peers):
        block = s_ref.at[lax.rem(an + answers - da, answers) * members + lax.rem(me + members - dm, members)]
        remote(block, block, s_send.at[i], s_recv.at[i], {"member": other}).wait_recv()
    for k, source in enumerate((an,) + sources):
        block = r_at(source, other)
        remote(block, block, f_send.at[k], f_recv.at[k], {"member": other}).wait_recv()
    for k, t in ((1, core), (2, 3 - te)):
        block = l_at(0, total, t)
        remote(block, block, y_send.at[k], y_recv.at[k], {"tensor": core}).wait_recv()
    own_r.wait()
    own_s.wait()
    for x in (2, 1):
        for c in range(len(chunks)):
            push(x, c).wait()
    for copy in [r_near, r_far, l_over, l_near, l_far, l_y, l_c, l_d] + scores + list(forward.values()):
        copy.wait_send()
    for copy in list(r_relays.values()) + list(l_relays.values()):
        pl.when(inner)(copy.wait_send)
    early.wait_recv()
    early.wait_send()


def exchange(left_noise, right_noise, returns, transposed, members, chunks):
    answers, sides = 4, 3
    local, width = right_noise.shape
    cols, tile = transposed.shape
    total = local * members * answers
    count = members * answers
    block = returns.shape[0]
    half = left_noise.dtype
    dma = pltpu.SemaphoreType.DMA
    vmem, anywhere = pl.BlockSpec(memory_space=pltpu.VMEM), pl.BlockSpec(memory_space=pl.ANY)
    shape = jax.ShapeDtypeStruct
    return pl.pallas_call(
        lambda *refs: exchange_kernel(members, chunks, *refs),
        out_shape=(
            shape((total, tile), half),
            shape((total, width), half),
            shape((count, 1, block), jnp.float32),
            shape((1, block), jnp.float32),
            shape((cols, chunks[0]), half),
        ) + tuple(shape((cols, size), half) for _ in range(sides) for size in chunks),
        in_specs=[vmem] * 3 + [anywhere],
        out_specs=(anywhere,) * (5 + sides * len(chunks)),
        scratch_shapes=[
            pltpu.VMEM((2, cols, tile // answers), jnp.float32), pltpu.VMEM((2, cols, tile // answers), half),
            pltpu.VMEM((1, block), jnp.float32),
            dma((4,)), dma((sides,)), dma((sides, len(chunks))), dma((count - 1,)), dma((count - 1,)),
            dma((1,)), dma((1,)), dma((answers,)), dma((answers,)),
            dma((4,)), dma((3,)), dma((4,)), dma((3,)), dma((3,)), dma((3,)), dma, dma,
        ],
        compiler_params=pltpu.CompilerParams(collective_id=0, has_side_effects=True),
        name="exchange",
    )(left_noise, right_noise, returns, transposed)


def divisor(size, least, most):
    fits = [n for n in range(least, most + 1, least) if size % n == 0]
    return fits[-1] if fits else size


def final_kernel(where_ref, master_ref, one_ref, two_ref, three_ref, left_ref, right_ref, *refs):
    out_ref, stack = refs[-2:]
    an = lax.axis_index("answer")
    width, rows = master_ref.shape
    near = an + 1 - 2 * lax.rem(an, 2)
    parts = ((an, master_ref), (near, one_ref), (lax.rem(an + 2, 4), two_ref), (3 - an, three_ref))
    for a, ref in parts:
        stack[pl.ds(pl.multiple_of(a * width, 16), width), :] = ref[...].astype(stack.dtype)
    row = lax.broadcasted_iota(jnp.int32, (rows, rows), 0)
    col = lax.broadcasted_iota(jnp.int32, (rows, rows), 1)
    unit = jnp.where(row == col, 1.0, 0.0).astype(stack.dtype)
    step = divisor(out_ref.shape[1], 128, 512)
    for at in range(0, out_ref.shape[1], step):
        cols = slice(at, at + step)
        new = jnp.dot(left_ref[...], right_ref[:, cols], preferred_element_type=jnp.float32)
        old = lax.dot_general(unit, stack[cols, :], (((1,), (1,)), ((), ())), preferred_element_type=jnp.float32)
        out_ref[:, cols] = (new + old).astype(out_ref.dtype)


def finalize(where, transposed, sides, left, right, first, size, so_far):
    rows, members = left.shape
    width = transposed.shape[0]
    total = right.shape[1]
    chunk = 128
    start, steps = first // chunk, size // chunk
    per = rows // chunk
    side = pl.BlockSpec((width, chunk), lambda i, w: (0, i))
    more = [] if so_far is None else [so_far]
    return pl.pallas_call(
        final_kernel,
        grid_spec=pltpu.PrefetchScalarGridSpec(
            num_scalar_prefetch=1,
            grid=(steps,),
            in_specs=[
                pl.BlockSpec((width, chunk), lambda i, w: (0, w[0] * per + start + i)),
                side, side, side,
                pl.BlockSpec((chunk, members), lambda i, w: (start + i, 0)),
                pl.BlockSpec((members, total), lambda i, w: (0, 0)),
            ] + [pl.BlockSpec(memory_space=pl.ANY)] * len(more),
            out_specs=pl.BlockSpec((chunk, total), lambda i, w: (start + i, 0)),
            scratch_shapes=[pltpu.VMEM((total, chunk), jnp.bfloat16)],
        ),
        out_shape=jax.ShapeDtypeStruct((rows, total), jnp.bfloat16),
        input_output_aliases={7: 0} if more else {},
        cost_estimate=pl.CostEstimate(
            flops=2 * size * total * (members + chunk), bytes_accessed=6 * size * total, transcendentals=0),
        name="final",
    )(where, transposed, *sides, left, right, *more)


def update_kernel(master_ref, right_ref, left_ref, new_ref):
    new_ref[...] = master_ref[...] + jnp.dot(right_ref[...], left_ref[...], preferred_element_type=jnp.float32)


def update(transposed, right, left):
    width, tile = transposed.shape
    members = right.shape[1]
    chunk = divisor(width, 16, 150)
    return pl.pallas_call(
        update_kernel,
        grid=(width // chunk,),
        in_specs=[
            pl.BlockSpec((chunk, tile), lambda i: (i, 0)),
            pl.BlockSpec((chunk, members), lambda i: (i, 0)),
            pl.BlockSpec((members, tile), lambda i: (0, 0)),
        ],
        out_specs=pl.BlockSpec((chunk, tile), lambda i: (i, 0)),
        out_shape=jax.ShapeDtypeStruct(transposed.shape, jnp.float32),
        cost_estimate=pl.CostEstimate(
            flops=2 * width * tile * members, bytes_accessed=8 * width * tile, transcendentals=0),
        name="update",
    )(transposed, right, left)


def weigh_kernel(members, l_ref, r_ref, s_ref, w_ref, o_ref, t_ref, turned):
    answers, block = s_ref.shape[0] // members, s_ref.shape[2]
    population = members * block
    local = block // answers
    an = lax.axis_index("answer")
    scores = []
    for m in range(members):
        total = s_ref[m]
        for a in range(1, answers):
            total = total + s_ref[a * members + m]
        scores.append(total)
    average = sum(jnp.sum(x, axis=1, keepdims=True) for x in scores) / population
    squares = sum(jnp.sum(x * x, axis=1, keepdims=True) for x in scores) / population
    spread = jnp.sqrt(squares - average * average + 1e-05) * jnp.sqrt(jnp.float32(population))
    for m in range(members):
        scale = jnp.broadcast_to((scores[m] - average) / spread, (block, block)).T[:, :1]
        for a in range(answers):
            at = (a * members + m) * local
            rows = slice(at, at + local)
            w_ref[rows, :] = (l_ref[rows, :].astype(jnp.float32) * scale[a * local:(a + 1) * local]).astype(w_ref.dtype)
    rows = o_ref.shape[0]
    o_ref[...] = w_ref[:, pl.ds(pl.multiple_of(an * rows, 128), rows)].T
    turned[...] = r_ref[...].T
    width = t_ref.shape[0]
    t_ref[...] = turned[pl.ds(pl.multiple_of(an * width, 16), width), :]


def weigh(left_tile, right, parts, members, rows, width):
    vmem = pl.BlockSpec(memory_space=pltpu.VMEM)
    total = left_tile.shape[0]
    half = left_tile.dtype
    return pl.pallas_call(
        lambda *refs: weigh_kernel(members, *refs),
        out_shape=(
            jax.ShapeDtypeStruct(left_tile.shape, half),
            jax.ShapeDtypeStruct((rows, total), half),
            jax.ShapeDtypeStruct((width, total), half),
        ),
        in_specs=[vmem] * 3,
        out_specs=(vmem,) * 3,
        scratch_shapes=[pltpu.VMEM(right.shape[::-1], half)],
        cost_estimate=pl.CostEstimate(flops=total * right.shape[1] * 256, bytes_accessed=1 << 23, transcendentals=0),
        name="weigh",
    )(left_tile, right, parts)


def split(rows):
    steps = rows // 128
    last = 1 if steps > 1 else 0
    first = (steps - last + 1) // 2
    return [n * 128 for n in (first, steps - last - first, last) if n]


def order_of(chunks):
    return [(c, x) for c in range(len(chunks)) for x in (2, 1, 3) if (c, x) != (0, 3)]


def fast_body(master, left_noise, right_noise, returns):
    members, answers = lax.axis_size("member"), lax.axis_size("answer")
    where = lax.axis_index("answer").astype(jnp.int32)[None]
    transposed = master.T
    width, tile = transposed.shape
    rows = tile // answers
    chunks = split(rows)
    left_tile, right, parts, _, early, *blocks = exchange(left_noise, right_noise, returns, transposed, members, chunks)
    blocks = [blocks[i:i + len(chunks)] for i in range(0, len(blocks), len(chunks))]
    got = {(0, 3): early}
    for c, x in order_of(chunks):
        got[c, x] = lax.ppermute(blocks[x - 1][c], "answer", [(i, i ^ x) for i in range(answers)])
    weighted, own, turned = weigh(left_tile, right, parts, members, rows, width)
    new_master = update(transposed, turned, weighted)
    rollout, at = None, 0
    for c, size in enumerate(chunks):
        rollout = finalize(where, transposed, [got[c, x] for x in (1, 2, 3)], own, right, at, size, rollout)
        at += size
    return (new_master.T, rollout)


def fits(members, tensors, answers, tile, local):
    return (members, tensors, answers) == (2, 4, 4) and tile % 512 == 0 and local % 32 == 0


def body(master, left_noise, right_noise, returns):
    sizes = [lax.axis_size(n) for n in ("member", "tensor", "answer")]
    fast = fits(*sizes, master.shape[0], left_noise.shape[0])
    return (fast_body if fast else plain_body)(master, left_noise, right_noise, returns)


def solution(mesh):
    return jax.shard_map(
        body,
        mesh=mesh,
        in_specs=(
            P("member", ("tensor", "answer")),
            P(("member", "answer"), None),
            P(("member", "answer"), "tensor"),
            P("member", "answer"),
        ),
        out_specs=(P("member", ("tensor", "answer")), P(("member", "answer"), "tensor")),
        check_vma=False,
    )
```

```python
import jax
import jax.numpy as jnp
from jax import lax
from jax.experimental import pallas as pl
from jax.experimental.pallas import tpu as pltpu
from jax.sharding import PartitionSpec as P


def contract(left_tile, accum, pieces):
    right_cols, weights = pieces
    weighted = left_tile.astype(jnp.float32) * weights[:, None]
    return accum + lax.dot_general(
        weighted,
        right_cols.astype(jnp.float32),
        (((0,), (0,)), ((), ())),
        precision=lax.Precision.HIGHEST,
    )


def plain_body(master, left_noise, right_noise, returns):
    member_count = lax.axis_size("member")
    answer_count = lax.axis_size("answer")
    partial_value = jnp.sum(returns, axis=1)
    block_len = partial_value.shape[0]
    population = block_len * member_count
    scores = lax.psum(partial_value, "answer")
    score_sum, square_sum = lax.psum((jnp.sum(scores), jnp.sum(scores * scores)), "member")
    average = score_sum / population
    variance = square_sum / population - average * average
    fitness = (scores - average) / jnp.sqrt(variance + 1e-05)
    tile_rows = master.shape[0]
    local_members = left_noise.shape[0]
    restricted = lax.all_to_all(left_noise, "member", split_axis=1, concat_axis=0, tiled=True)
    gathered_rows = lax.all_gather(restricted, "answer", axis=0, tiled=True)
    width = gathered_rows.shape[1]
    left_tile = gathered_rows.reshape(answer_count, member_count, local_members, width)
    left_tile = jnp.transpose(left_tile, (1, 0, 2, 3)).reshape(
        answer_count * member_count * local_members, width
    )
    right_block = lax.all_to_all(right_noise, "answer", split_axis=1, concat_axis=0, tiled=True)
    initial = jnp.zeros((tile_rows, right_block.shape[1]), jnp.float32)
    update = contract(
        left_tile,
        initial,
        (
            lax.all_gather(right_block, "member", axis=0, tiled=True),
            lax.all_gather(fitness.astype(jnp.bfloat16), "member", axis=0, tiled=True).astype(
                jnp.float32
            ),
        ),
    )
    new_master = master + update / jnp.sqrt(jnp.float32(population))
    rollout = lax.all_to_all(
        new_master.astype(jnp.bfloat16), "answer", split_axis=0, concat_axis=1, tiled=True
    )
    return (new_master, rollout)


def exchange_kernel(members, chunks, left_ref, right_ref, returns_ref, master_ref, *refs):
    sides = 3
    l_ref, r_ref, s_ref, p_ref, e_ref, *refs = refs
    blocks, refs = refs[:sides * len(chunks)], refs[sides * len(chunks):]
    (wide, narrow, part, own_sem, pull_sem, push_sem, s_send, s_recv, x_send, x_recv, f_send, f_recv,
     z_send, z_recv, q_send, q_recv, y_send, y_recv, e_send, e_recv) = refs
    me, te, an = lax.axis_index("member"), lax.axis_index("tensor"), lax.axis_index("answer")
    answers = 4
    local = left_ref.shape[0]
    slab = local * members
    tile = l_ref.shape[1]
    piece = tile // 4
    rows = tile // answers
    beside = lambda i: i + 1 - 2 * lax.rem(i, 2)
    other, core, across = 1 - me, beside(te), lax.rem(te + 2, 4)
    near, far = beside(an), 2 - lax.div(an, 2)
    beyond = 2 * (1 - lax.div(an, 2))
    inner = lax.div(an + 1, 2) == 1
    pair = {1: near, 2: lax.rem(an + 2, answers), 3: answers - 1 - an}

    def l_at(start, count, t):
        return l_ref.at[pl.ds(pl.multiple_of(start, local), count), pl.ds(pl.multiple_of(t * piece, piece), piece)]

    def l_slab(a, t):
        return l_at(a * slab, slab, t)

    def r_at(a, m):
        return r_ref.at[pl.ds(pl.multiple_of((a * members + m) * local, local), local), :]

    def remote(src, dst, send, recv, where):
        return pltpu.make_async_remote_copy(src_ref=src, dst_ref=dst, send_sem=send, recv_sem=recv,
                                            device_id=where, device_id_type=pl.DeviceIdType.MESH)

    def pull(x):
        return pltpu.make_async_copy(
            master_ref.at[:, pl.ds(pl.multiple_of(pair[x] * rows, rows), rows)], wide.at[x % 2], pull_sem.at[x - 1])

    def push(x, c):
        at = sum(chunks[:c])
        return pltpu.make_async_copy(
            narrow.at[x % 2, :, at:at + chunks[c]], blocks[(x - 1) * len(chunks) + c], push_sem.at[x - 1, c])

    def cast(x):
        pull(x).wait()
        step = 96

        def one(i, _):
            at = pl.ds(pl.multiple_of(i * step, step), step)
            narrow[x % 2, at, :] = wide[x % 2, at, :].astype(narrow.dtype)
            return 0

        lax.fori_loop(0, narrow.shape[1] // step, one, 0)
        for c in range(len(chunks)):
            push(x, c).start()

    barrier = pltpu.get_barrier_semaphore()
    peers = [(dm, da) for dm in range(members) for da in range(answers) if (dm, da) != (0, 0)]
    place = lambda dm, da: {"member": lax.rem(me + dm, members), "answer": lax.rem(an + da, answers)}
    for dm, da in peers:
        pl.semaphore_signal(barrier, inc=1, device_id=place(dm, da), device_id_type=pl.DeviceIdType.MESH)
    for t in (core, across):
        pl.semaphore_signal(barrier, inc=1, device_id={"tensor": t}, device_id_type=pl.DeviceIdType.MESH)
    pull(3).start()
    pull(2).start()
    own_l = pltpu.make_async_copy(
        left_ref.at[:, pl.ds(pl.multiple_of(me * tile + te * piece, piece), piece)],
        l_at((an * members + me) * local, local, te), own_sem.at[0])
    own_r = pltpu.make_async_copy(right_ref, r_at(an, me), own_sem.at[1])
    own_l.start()
    own_r.start()
    part[...] = jnp.sum(returns_ref[...].T, axis=0, keepdims=True)
    own_p = pltpu.make_async_copy(part, p_ref, own_sem.at[2])
    own_s = pltpu.make_async_copy(part, s_ref.at[an * members + me], own_sem.at[3])
    own_p.start()
    own_s.start()

    pl.semaphore_wait(barrier, len(peers) + 2)

    mine = lax.rem(an, 2)
    halves = 2
    count = local // halves
    sources = (an, near, beyond, beyond + 1)
    started = []

    def start(copy):
        copy.start()
        started.append(copy)
        return copy

    def landed(block, sem):
        remote(block, block, x_send.at[0], sem, {"member": other}).wait_recv()

    def r_half(a, m, h):
        return r_ref.at[pl.ds(pl.multiple_of((a * members + m) * local + h * count, count), count), :]

    def forward(k, h):
        block = r_half(sources[k], me, h)
        src = right_ref.at[h * count:(h + 1) * count, :] if k == 0 else block
        start(remote(src, block, f_send.at[k, h], f_recv.at[k, h], {"member": other}))

    def spread(k):
        block = l_slab(sources[k], te)
        start(remote(block, block, y_send.at[k, 0], y_recv.at[k, 0], {"tensor": across}))
        start(remote(block, block, y_send.at[k, 1], y_recv.at[k, 1], {"tensor": core}))

    start(remote(left_ref.at[:, pl.ds(pl.multiple_of(other * tile + te * piece, piece), piece)],
                 l_at((an * members + me) * local, local, te), x_send.at[0], x_recv.at[0], {"member": other}))

    def part_of(h):
        src = right_ref.at[h * count:(h + 1) * count, :]
        start(remote(src, r_half(an, me, h), z_send.at[0, h], z_recv.at[1 + mine, h], {"answer": far}))
        start(remote(src, r_half(an, me, h), z_send.at[1, h], z_recv.at[0, h], {"answer": near}))

    part_of(0)
    own_p.wait()
    for i, (dm, da) in enumerate(peers):
        start(remote(p_ref, s_ref.at[an * members + me], s_send.at[i], s_recv.at[i], place(dm, da)))
    own_l.wait()
    landed(l_at((an * members + other) * local, local, te), x_recv.at[0])
    block = l_slab(an, te)
    start(remote(block, block, q_send.at[0], q_recv.at[1 + mine], {"answer": far}))
    start(remote(block, block, q_send.at[1], q_recv.at[0], {"answer": near}))
    part_of(1)
    spread(0)
    for h in range(halves):
        forward(0, h)
    cast(3)
    early = []
    for c, size in enumerate(chunks):
        push(3, c).wait()
        at = sum(chunks[:c])
        copy = remote(blocks[2 * len(chunks) + c], e_ref.at[:, at:at + size], e_send.at[c], e_recv.at[c], {"answer": pair[3]})
        pl.when(inner)(copy.start)
        early.append(copy)
    pull(1).start()
    for h in range(halves):
        landed(r_half(near, me, h), z_recv.at[0, h])
        forward(1, h)
    landed(l_slab(near, te), q_recv.at[0])
    spread(1)
    cast(2)
    relays = []

    def relay(block, send, recv):
        copy = remote(block, block, send, recv, {"answer": near})
        pl.when(inner)(copy.start)
        relays.append(copy)

    def pass_on(h):
        for k in (2, 3):
            block = r_half(sources[k], me, h)
            landed(block, z_recv.at[k - 1, h])
            relay(block, z_send.at[k, h], z_recv.at[k - 1, h])
            forward(k, h)

    pass_on(0)
    for k in (2, 3):
        block = l_slab(sources[k], te)
        landed(block, q_recv.at[k - 1])
        relay(block, q_send.at[k], q_recv.at[k - 1])
        spread(k)
    pass_on(1)
    for k in range(answers):
        block = l_slab(sources[k], across)
        landed(block, y_recv.at[k, 0])
        start(remote(block, block, y_send.at[k, 2], y_recv.at[k, 2], {"tensor": core}))
    cast(1)
    for i, (dm, da) in enumerate(peers):
        landed(s_ref.at[lax.rem(an + answers - da, answers) * members + lax.rem(me + members - dm, members)], s_recv.at[i])
    for k in range(answers):
        for h in range(halves):
            landed(r_half(sources[k], other, h), f_recv.at[k, h])
    for k in range(answers):
        landed(l_slab(sources[k], core), y_recv.at[k, 1])
        landed(l_slab(sources[k], 3 - te), y_recv.at[k, 2])
    own_r.wait()
    own_s.wait()
    for x in (2, 1):
        for c in range(len(chunks)):
            push(x, c).wait()
    for copy in started:
        copy.wait_send()
    for copy in relays + early:
        pl.when(inner)(copy.wait_send)
    for copy in early:
        pl.when(inner)(copy.wait_recv)


def exchange(left_noise, right_noise, returns, transposed, members, chunks):
    answers, sides = 4, 3
    local, width = right_noise.shape
    cols, tile = transposed.shape
    total = local * members * answers
    count = members * answers
    block = returns.shape[0]
    half = left_noise.dtype
    dma = pltpu.SemaphoreType.DMA
    vmem, anywhere = pl.BlockSpec(memory_space=pltpu.VMEM), pl.BlockSpec(memory_space=pl.ANY)
    shape = jax.ShapeDtypeStruct
    return pl.pallas_call(
        lambda *refs: exchange_kernel(members, chunks, *refs),
        out_shape=(
            shape((total, tile), half),
            shape((total, width), half),
            shape((count, 1, block), jnp.float32),
            shape((1, block), jnp.float32),
            shape((cols, tile // answers), half),
        ) + tuple(shape((cols, size), half) for _ in range(sides) for size in chunks),
        in_specs=[vmem] * 3 + [anywhere],
        out_specs=(anywhere,) * (5 + sides * len(chunks)),
        scratch_shapes=[
            pltpu.VMEM((2, cols, tile // answers), jnp.float32), pltpu.VMEM((2, cols, tile // answers), half),
            pltpu.VMEM((1, block), jnp.float32),
            dma((4,)), dma((sides,)), dma((sides, len(chunks))), dma((count - 1,)), dma((count - 1,)),
            dma((1,)), dma((1,)), dma((answers, 2)), dma((answers, 2)),
            dma((4, 2)), dma((3, 2)), dma((4,)), dma((3,)), dma((answers, 3)), dma((answers, 3)),
            dma((len(chunks),)), dma((len(chunks),)),
        ],
        compiler_params=pltpu.CompilerParams(collective_id=0, has_side_effects=True),
        name="exchange",
    )(left_noise, right_noise, returns, transposed)


def divisor(size, least, most):
    fits = [n for n in range(least, most + 1, least) if size % n == 0]
    return fits[-1] if fits else size


def final_kernel(where_ref, master_ref, one_ref, two_ref, three_ref, early_ref, left_ref, right_ref, *refs):
    out_ref, stack = refs[-2:]
    an = lax.axis_index("answer")
    width, rows = master_ref.shape
    near = an + 1 - 2 * lax.rem(an, 2)
    inner = lax.div(an + 1, 2) == 1

    def place(a, ref):
        stack[pl.ds(pl.multiple_of(a * width, 16), width), :] = ref[...].astype(stack.dtype)

    place(an, master_ref)
    place(near, one_ref)
    place(lax.rem(an + 2, 4), two_ref)
    pl.when(inner)(lambda: place(3 - an, early_ref))
    pl.when(jnp.logical_not(inner))(lambda: place(3 - an, three_ref))
    row = lax.broadcasted_iota(jnp.int32, (rows, rows), 0)
    col = lax.broadcasted_iota(jnp.int32, (rows, rows), 1)
    unit = jnp.where(row == col, 1.0, 0.0).astype(stack.dtype)
    step = divisor(out_ref.shape[1], 128, 512)
    for at in range(0, out_ref.shape[1], step):
        cols = slice(at, at + step)
        new = jnp.dot(left_ref[...], right_ref[:, cols], preferred_element_type=jnp.float32)
        old = lax.dot_general(unit, stack[cols, :], (((1,), (1,)), ((), ())), preferred_element_type=jnp.float32)
        out_ref[:, cols] = (new + old).astype(out_ref.dtype)


def finalize(where, transposed, sides, early, left, right, first, size, so_far):
    rows, members = left.shape
    width = transposed.shape[0]
    total = right.shape[1]
    chunk = 128
    start, steps = first // chunk, size // chunk
    per = rows // chunk
    side = pl.BlockSpec((width, chunk), lambda i, w: (0, i))
    more = [] if so_far is None else [so_far]
    return pl.pallas_call(
        final_kernel,
        grid_spec=pltpu.PrefetchScalarGridSpec(
            num_scalar_prefetch=1,
            grid=(steps,),
            in_specs=[
                pl.BlockSpec((width, chunk), lambda i, w: (0, w[0] * per + start + i)),
                side, side, side,
                pl.BlockSpec((width, chunk), lambda i, w: (0, start + i)),
                pl.BlockSpec((chunk, members), lambda i, w: (start + i, 0)),
                pl.BlockSpec((members, total), lambda i, w: (0, 0)),
            ] + [pl.BlockSpec(memory_space=pl.ANY)] * len(more),
            out_specs=pl.BlockSpec((chunk, total), lambda i, w: (start + i, 0)),
            scratch_shapes=[pltpu.VMEM((total, chunk), jnp.bfloat16)],
        ),
        out_shape=jax.ShapeDtypeStruct((rows, total), jnp.bfloat16),
        input_output_aliases={8: 0} if more else {},
        cost_estimate=pl.CostEstimate(
            flops=2 * size * total * (members + chunk), bytes_accessed=6 * size * total, transcendentals=0),
        compiler_params=pltpu.CompilerParams(vmem_limit_bytes=24 << 20),
        name="final",
    )(where, transposed, *sides, early, left, right, *more)


def update_kernel(master_ref, right_ref, left_ref, new_ref):
    new_ref[...] = master_ref[...] + jnp.dot(right_ref[...], left_ref[...], preferred_element_type=jnp.float32)


def update(transposed, right, left):
    width, tile = transposed.shape
    members = right.shape[1]
    chunk = divisor(width, 16, 150)
    return pl.pallas_call(
        update_kernel,
        grid=(width // chunk,),
        in_specs=[
            pl.BlockSpec((chunk, tile), lambda i: (i, 0)),
            pl.BlockSpec((chunk, members), lambda i: (i, 0)),
            pl.BlockSpec((members, tile), lambda i: (0, 0)),
        ],
        out_specs=pl.BlockSpec((chunk, tile), lambda i: (i, 0)),
        out_shape=jax.ShapeDtypeStruct(transposed.shape, jnp.float32),
        cost_estimate=pl.CostEstimate(
            flops=2 * width * tile * members, bytes_accessed=8 * width * tile, transcendentals=0),
        compiler_params=pltpu.CompilerParams(vmem_limit_bytes=24 << 20),
        name="update",
    )(transposed, right, left)


def weigh_kernel(members, l_ref, r_ref, s_ref, w_ref, o_ref, t_ref, turned):
    answers, block = s_ref.shape[0] // members, s_ref.shape[2]
    population = members * block
    local = block // answers
    an = lax.axis_index("answer")
    scores = []
    for m in range(members):
        total = s_ref[m]
        for a in range(1, answers):
            total = total + s_ref[a * members + m]
        scores.append(total)
    average = sum(jnp.sum(x, axis=1, keepdims=True) for x in scores) / population
    squares = sum(jnp.sum(x * x, axis=1, keepdims=True) for x in scores) / population
    spread = jnp.sqrt(squares - average * average + 1e-05) * jnp.sqrt(jnp.float32(population))
    for m in range(members):
        scale = jnp.broadcast_to((scores[m] - average) / spread, (block, block)).T[:, :1]
        for a in range(answers):
            at = (a * members + m) * local
            rows = slice(at, at + local)
            w_ref[rows, :] = (l_ref[rows, :].astype(jnp.float32) * scale[a * local:(a + 1) * local]).astype(w_ref.dtype)
    rows = o_ref.shape[0]
    o_ref[...] = w_ref[:, pl.ds(pl.multiple_of(an * rows, 128), rows)].T
    turned[...] = r_ref[...].T
    width = t_ref.shape[0]
    t_ref[...] = turned[pl.ds(pl.multiple_of(an * width, 16), width), :]


def weigh(left_tile, right, parts, members, rows, width):
    vmem = pl.BlockSpec(memory_space=pltpu.VMEM)
    total = left_tile.shape[0]
    half = left_tile.dtype
    return pl.pallas_call(
        lambda *refs: weigh_kernel(members, *refs),
        out_shape=(
            jax.ShapeDtypeStruct(left_tile.shape, half),
            jax.ShapeDtypeStruct((rows, total), half),
            jax.ShapeDtypeStruct((width, total), half),
        ),
        in_specs=[vmem] * 3,
        out_specs=(vmem,) * 3,
        scratch_shapes=[pltpu.VMEM(right.shape[::-1], half)],
        cost_estimate=pl.CostEstimate(flops=total * right.shape[1] * 256, bytes_accessed=1 << 23, transcendentals=0),
        compiler_params=pltpu.CompilerParams(vmem_limit_bytes=24 << 20),
        name="weigh",
    )(left_tile, right, parts)


def split(rows):
    steps = rows // 128
    last = 1 if steps > 1 else 0
    first = (steps - last + 1) // 2
    return [n * 128 for n in (first, steps - last - first, last) if n]


def order_of(count):
    return [(c, x) for c in range(count) for x in (3, 2, 1)]


def fast_body(master, left_noise, right_noise, returns):
    members, answers = lax.axis_size("member"), lax.axis_size("answer")
    where = lax.axis_index("answer").astype(jnp.int32)[None]
    transposed = master.T
    width, tile = transposed.shape
    rows = tile // answers
    chunks = split(rows)
    left_tile, right, parts, _, early, *blocks = exchange(left_noise, right_noise, returns, transposed, members, chunks)
    blocks = [blocks[i:i + len(chunks)] for i in range(0, len(blocks), len(chunks))]
    got = {}
    for c, x in order_of(len(chunks)):
        got[c, x] = lax.ppermute(blocks[x - 1][c], "answer", [(i, i ^ x) for i in range(answers) if x < 3 or i in (0, 3)])
    weighted, own, turned = weigh(left_tile, right, parts, members, rows, width)
    new_master = update(transposed, turned, weighted)
    rollout, at = None, 0
    for c, size in enumerate(chunks):
        rollout = finalize(where, transposed, [got[c, x] for x in (1, 2, 3)], early, own, right, at, size, rollout)
        at += size
    return (new_master.T, rollout)


def fits(members, tensors, answers, tile, local):
    return (members, tensors, answers) == (2, 4, 4) and tile % 512 == 0 and local % 32 == 0


def body(master, left_noise, right_noise, returns):
    sizes = [lax.axis_size(n) for n in ("member", "tensor", "answer")]
    fast = fits(*sizes, master.shape[0], left_noise.shape[0])
    return (fast_body if fast else plain_body)(master, left_noise, right_noise, returns)


def solution(mesh):
    return jax.shard_map(
        body,
        mesh=mesh,
        in_specs=(
            P("member", ("tensor", "answer")),
            P(("member", "answer"), None),
            P(("member", "answer"), "tensor"),
            P("member", "answer"),
        ),
        out_specs=(P("member", ("tensor", "answer")), P(("member", "answer"), "tensor")),
        check_vma=False,
    )
```

```python
import jax
import jax.numpy as jnp
from jax import lax
from jax.experimental import pallas as pl
from jax.experimental.pallas import tpu as pltpu
from jax.sharding import PartitionSpec as P


def contract(left_tile, accum, pieces):
    right_cols, weights = pieces
    weighted = left_tile.astype(jnp.float32) * weights[:, None]
    return accum + lax.dot_general(
        weighted,
        right_cols.astype(jnp.float32),
        (((0,), (0,)), ((), ())),
        precision=lax.Precision.HIGHEST,
    )


def plain_body(master, left_noise, right_noise, returns):
    member_count = lax.axis_size("member")
    answer_count = lax.axis_size("answer")
    partial_value = jnp.sum(returns, axis=1)
    block_len = partial_value.shape[0]
    population = block_len * member_count
    scores = lax.psum(partial_value, "answer")
    score_sum, square_sum = lax.psum((jnp.sum(scores), jnp.sum(scores * scores)), "member")
    average = score_sum / population
    variance = square_sum / population - average * average
    fitness = (scores - average) / jnp.sqrt(variance + 1e-05)
    tile_rows = master.shape[0]
    local_members = left_noise.shape[0]
    restricted = lax.all_to_all(left_noise, "member", split_axis=1, concat_axis=0, tiled=True)
    gathered_rows = lax.all_gather(restricted, "answer", axis=0, tiled=True)
    width = gathered_rows.shape[1]
    left_tile = gathered_rows.reshape(answer_count, member_count, local_members, width)
    left_tile = jnp.transpose(left_tile, (1, 0, 2, 3)).reshape(
        answer_count * member_count * local_members, width
    )
    right_block = lax.all_to_all(right_noise, "answer", split_axis=1, concat_axis=0, tiled=True)
    initial = jnp.zeros((tile_rows, right_block.shape[1]), jnp.float32)
    update = contract(
        left_tile,
        initial,
        (
            lax.all_gather(right_block, "member", axis=0, tiled=True),
            lax.all_gather(fitness.astype(jnp.bfloat16), "member", axis=0, tiled=True).astype(
                jnp.float32
            ),
        ),
    )
    new_master = master + update / jnp.sqrt(jnp.float32(population))
    rollout = lax.all_to_all(
        new_master.astype(jnp.bfloat16), "answer", split_axis=0, concat_axis=1, tiled=True
    )
    return (new_master, rollout)


def exchange_kernel(members, chunks, left_ref, right_ref, returns_ref, master_ref, *refs):
    sides = 3
    l_ref, r_ref, s_ref, p_ref, e_ref, n_ref, b_ref, *refs = refs
    blocks, refs = refs[:sides * len(chunks)], refs[sides * len(chunks):]
    (wide, narrow, part, own_sem, pull_sem, push_sem, s_send, s_recv, t_send, t_recv, x_send, x_recv, f_send, f_recv,
     z_send, z_recv, q_send, q_recv, y_send, y_recv, e_send, e_recv, n_send, n_recv, b_send, b_recv) = refs
    me, te, an = lax.axis_index("member"), lax.axis_index("tensor"), lax.axis_index("answer")
    answers = 4
    local = left_ref.shape[0]
    slab = local * members
    tile = l_ref.shape[1]
    piece = tile // 4
    rows = tile // answers
    beside = lambda i: i + 1 - 2 * lax.rem(i, 2)
    other, core, across = 1 - me, beside(te), lax.rem(te + 2, 4)
    near, far = beside(an), 2 - lax.div(an, 2)
    beyond = 2 * (1 - lax.div(an, 2))
    inner = lax.div(an + 1, 2) == 1
    outer = jnp.logical_not(inner)
    pair = {1: near, 2: lax.rem(an + 2, answers), 3: answers - 1 - an}

    def l_at(start, count, t):
        return l_ref.at[pl.ds(pl.multiple_of(start, local), count), pl.ds(pl.multiple_of(t * piece, piece), piece)]

    def l_slab(a, t):
        return l_at(a * slab, slab, t)

    def r_at(a, m):
        return r_ref.at[pl.ds(pl.multiple_of((a * members + m) * local, local), local), :]

    def remote(src, dst, send, recv, where):
        return pltpu.make_async_remote_copy(src_ref=src, dst_ref=dst, send_sem=send, recv_sem=recv,
                                            device_id=where, device_id_type=pl.DeviceIdType.MESH)

    def pull(x):
        return pltpu.make_async_copy(
            master_ref.at[:, pl.ds(pl.multiple_of(pair[x] * rows, rows), rows)], wide.at[x % 2], pull_sem.at[x - 1])

    def push(x, c):
        at = sum(chunks[:c])
        return pltpu.make_async_copy(
            narrow.at[x % 2, :, at:at + chunks[c]], blocks[(x - 1) * len(chunks) + c], push_sem.at[x - 1, c])

    def cast(x):
        pull(x).wait()
        step = 96

        def one(i, _):
            at = pl.ds(pl.multiple_of(i * step, step), step)
            narrow[x % 2, at, :] = wide[x % 2, at, :].astype(narrow.dtype)
            return 0

        lax.fori_loop(0, narrow.shape[1] // step, one, 0)
        for c in range(len(chunks)):
            push(x, c).start()

    barrier = pltpu.get_barrier_semaphore()

    def greet(where):
        pl.semaphore_signal(barrier, inc=1, device_id=where, device_id_type=pl.DeviceIdType.MESH)

    for where in ({"answer": near}, {"member": other}, {"tensor": core}, {"tensor": across}):
        greet(where)

    @pl.when(inner)
    def _():
        greet({"answer": beyond})
        greet({"answer": beyond + 1})

    pull(1).start()
    pull(2).start()
    own_l = pltpu.make_async_copy(
        left_ref.at[:, pl.ds(pl.multiple_of(me * tile + te * piece, piece), piece)],
        l_at((an * members + me) * local, local, te), own_sem.at[0])
    own_r = pltpu.make_async_copy(right_ref, r_at(an, me), own_sem.at[1])
    own_l.start()
    own_r.start()
    part[...] = jnp.sum(returns_ref[...].T, axis=0, keepdims=True)
    own_p = pltpu.make_async_copy(part, p_ref, own_sem.at[2])
    own_s = pltpu.make_async_copy(part, s_ref.at[an * members + me], own_sem.at[3])
    own_p.start()
    own_s.start()

    pl.semaphore_wait(barrier, 5)

    mine = lax.rem(an, 2)
    halves = 2
    count = local // halves
    sources = (an, near, beyond, beyond + 1)
    started = []

    def start(copy):
        copy.start()
        started.append(copy)
        return copy

    def landed(block, sem):
        remote(block, block, x_send.at[0], sem, {"member": other}).wait_recv()

    def r_half(a, m, h):
        return r_ref.at[pl.ds(pl.multiple_of((a * members + m) * local + h * count, count), count), :]

    def forward(k, h):
        block = r_half(sources[k], me, h)
        src = right_ref.at[h * count:(h + 1) * count, :] if k == 0 else block
        start(remote(src, block, f_send.at[k, h], f_recv.at[k, h], {"member": other}))

    def spread(k):
        block = l_slab(sources[k], te)
        start(remote(block, block, y_send.at[k, 0], y_recv.at[k, 0], {"tensor": across}))
        start(remote(block, block, y_send.at[k, 1], y_recv.at[k, 1], {"tensor": core}))

    start(remote(left_ref.at[:, pl.ds(pl.multiple_of(other * tile + te * piece, piece), piece)],
                 l_at((an * members + me) * local, local, te), x_send.at[0], x_recv.at[0], {"member": other}))

    def part_of(h):
        src = right_ref.at[h * count:(h + 1) * count, :]
        start(remote(src, r_half(an, me, h), z_send.at[0, h], z_recv.at[1 + mine, h], {"answer": far}))
        start(remote(src, r_half(an, me, h), z_send.at[1, h], z_recv.at[0, h], {"answer": near}))

    part_of(0)
    own_p.wait()
    score = lambda a, m: s_ref.at[a * members + m]
    start(remote(p_ref, score(an, me), s_send.at[0], s_recv.at[mine + 1], {"answer": far}))
    start(remote(p_ref, score(an, me), s_send.at[1], s_recv.at[0], {"answer": near}))
    start(remote(p_ref, score(an, me), t_send.at[0], t_recv.at[0], {"member": other}))
    own_l.wait()
    landed(l_at((an * members + other) * local, local, te), x_recv.at[0])
    block = l_slab(an, te)
    start(remote(block, block, q_send.at[0], q_recv.at[1 + mine], {"answer": far}))
    start(remote(block, block, q_send.at[1], q_recv.at[0], {"answer": near}))
    part_of(1)
    spread(0)
    for h in range(halves):
        forward(0, h)
    last = len(chunks) - 1
    cast(1)
    push(1, last).wait()
    aside = remote(blocks[last], b_ref, b_send, b_recv, {"answer": near})
    pl.when(inner)(aside.start)
    for c in range(last):
        push(1, c).wait()
    pull(3).start()
    cast(2)
    push(2, last).wait()
    cross = remote(blocks[len(chunks) + last], n_ref, n_send, n_recv, {"answer": far})
    pl.when(outer)(cross.start)
    cast(3)
    early = []
    push(3, last).wait()
    for c, size in enumerate(chunks[:last]):
        push(3, c).wait()
        at = sum(chunks[:c])
        copy = remote(blocks[2 * len(chunks) + c], e_ref.at[:, at:at + size], e_send.at[c], e_recv.at[c], {"answer": pair[3]})
        pl.when(inner)(copy.start)
        early.append(copy)
    for h in range(halves):
        landed(r_half(near, me, h), z_recv.at[0, h])
        forward(1, h)
    landed(l_slab(near, te), q_recv.at[0])
    spread(1)
    relays = []

    def relay(block, send, recv):
        copy = remote(block, block, send, recv, {"answer": near})
        pl.when(inner)(copy.start)
        relays.append(copy)

    def pass_on(h):
        for k in (2, 3):
            block = r_half(sources[k], me, h)
            landed(block, z_recv.at[k - 1, h])
            relay(block, z_send.at[k, h], z_recv.at[k - 1, h])
            forward(k, h)

    pass_on(0)
    for k in (2, 3):
        block = l_slab(sources[k], te)
        landed(block, q_recv.at[k - 1])
        relay(block, q_send.at[k], q_recv.at[k - 1])
        spread(k)
    pass_on(1)
    for k in range(answers):
        block = l_slab(sources[k], across)
        landed(block, y_recv.at[k, 0])
        start(remote(block, block, y_send.at[k, 2], y_recv.at[k, 2], {"tensor": core}))
    for k in range(1, answers):
        block = score(sources[k], me)
        landed(block, s_recv.at[k - 1])
        if k > 1:
            relay(block, s_send.at[k], s_recv.at[k - 1])
        start(remote(block, block, t_send.at[k], t_recv.at[k], {"member": other}))
    for k in range(answers):
        landed(score(sources[k], other), t_recv.at[k])
    for k in range(answers):
        for h in range(halves):
            landed(r_half(sources[k], other, h), f_recv.at[k, h])
    for k in range(answers):
        landed(l_slab(sources[k], core), y_recv.at[k, 1])
        landed(l_slab(sources[k], 3 - te), y_recv.at[k, 2])
    own_r.wait()
    own_s.wait()
    for c in range(last):
        push(2, c).wait()
    for copy in started:
        copy.wait_send()
    for copy in relays + early:
        pl.when(inner)(copy.wait_send)
    for copy in early:
        pl.when(inner)(copy.wait_recv)
    pl.when(outer)(cross.wait_send)
    pl.when(inner)(cross.wait_recv)
    pl.when(inner)(aside.wait_send)
    pl.when(outer)(aside.wait_recv)


def exchange(left_noise, right_noise, returns, transposed, members, chunks):
    answers, sides = 4, 3
    local, width = right_noise.shape
    cols, tile = transposed.shape
    total = local * members * answers
    count = members * answers
    block = returns.shape[0]
    half = left_noise.dtype
    dma = pltpu.SemaphoreType.DMA
    vmem, anywhere = pl.BlockSpec(memory_space=pltpu.VMEM), pl.BlockSpec(memory_space=pl.ANY)
    shape = jax.ShapeDtypeStruct
    return pl.pallas_call(
        lambda *refs: exchange_kernel(members, chunks, *refs),
        out_shape=(
            shape((total, tile), half),
            shape((total, width), half),
            shape((count, 1, block), jnp.float32),
            shape((1, block), jnp.float32),
            shape((cols, sum(chunks[:-1])), half),
            shape((cols, chunks[-1]), half),
            shape((cols, chunks[-1]), half),
        ) + tuple(shape((cols, size), half) for _ in range(sides) for size in chunks),
        in_specs=[vmem] * 3 + [anywhere],
        out_specs=(anywhere,) * (7 + sides * len(chunks)),
        scratch_shapes=[
            pltpu.VMEM((2, cols, tile // answers), jnp.float32), pltpu.VMEM((2, cols, tile // answers), half),
            pltpu.VMEM((1, block), jnp.float32),
            dma((4,)), dma((sides,)), dma((sides, len(chunks))), dma((4,)), dma((3,)), dma((4,)), dma((4,)),
            dma((1,)), dma((1,)), dma((answers, 2)), dma((answers, 2)),
            dma((4, 2)), dma((3, 2)), dma((4,)), dma((3,)), dma((answers, 3)), dma((answers, 3)),
            dma((len(chunks) - 1,)), dma((len(chunks) - 1,)), dma, dma, dma, dma,
        ],
        compiler_params=pltpu.CompilerParams(collective_id=0, has_side_effects=True),
        name="exchange",
    )(left_noise, right_noise, returns, transposed)


def divisor(size, least, most):
    fits = [n for n in range(least, most + 1, least) if size % n == 0]
    return fits[-1] if fits else size


def final_kernel(picks, where_ref, master_ref, *refs):
    sides, refs = refs[:len(picks)], refs[len(picks):]
    left_ref, right_ref, out_ref, stack = refs[0], refs[1], refs[-2], refs[-1]
    an = lax.axis_index("answer")
    width, rows = master_ref.shape
    near = an + 1 - 2 * lax.rem(an, 2)
    inner = lax.div(an + 1, 2) == 1
    places = {1: near, 2: lax.rem(an + 2, 4), 3: 3 - an}
    within = {True: inner, False: jnp.logical_not(inner)}

    def place(a, ref):
        stack[pl.ds(pl.multiple_of(a * width, 16), width), :] = ref[...].astype(stack.dtype)

    place(an, master_ref)
    for (x, which), ref in zip(picks, sides):
        if which is None:
            place(places[x], ref)
        else:
            pl.when(within[which])(lambda x=x, ref=ref: place(places[x], ref))
    row = lax.broadcasted_iota(jnp.int32, (rows, rows), 0)
    col = lax.broadcasted_iota(jnp.int32, (rows, rows), 1)
    unit = jnp.where(row == col, 1.0, 0.0).astype(stack.dtype)
    step = divisor(out_ref.shape[1], 128, 512)
    for at in range(0, out_ref.shape[1], step):
        cols = slice(at, at + step)
        new = jnp.dot(left_ref[...], right_ref[:, cols], preferred_element_type=jnp.float32)
        old = lax.dot_general(unit, stack[cols, :], (((1,), (1,)), ((), ())), preferred_element_type=jnp.float32)
        out_ref[:, cols] = (new + old).astype(out_ref.dtype)


def finalize(where, transposed, sides, left, right, first, size, so_far):
    rows, members = left.shape
    width = transposed.shape[0]
    total = right.shape[1]
    chunk = 128
    start, steps = first // chunk, size // chunk
    per = rows // chunk
    more = [] if so_far is None else [so_far]
    picks = tuple(key for key, _, _ in sides)
    blocks = [pl.BlockSpec((width, chunk), lambda i, w, at=at: (0, at + i)) for _, _, at in sides]
    return pl.pallas_call(
        lambda *refs: final_kernel(picks, *refs),
        grid_spec=pltpu.PrefetchScalarGridSpec(
            num_scalar_prefetch=1,
            grid=(steps,),
            in_specs=[pl.BlockSpec((width, chunk), lambda i, w: (0, w[0] * per + start + i))] + blocks + [
                pl.BlockSpec((chunk, members), lambda i, w: (start + i, 0)),
                pl.BlockSpec((members, total), lambda i, w: (0, 0)),
            ] + [pl.BlockSpec(memory_space=pl.ANY)] * len(more),
            out_specs=pl.BlockSpec((chunk, total), lambda i, w: (start + i, 0)),
            scratch_shapes=[pltpu.VMEM((total, chunk), jnp.bfloat16)],
        ),
        out_shape=jax.ShapeDtypeStruct((rows, total), jnp.bfloat16),
        input_output_aliases={4 + len(sides): 0} if more else {},
        cost_estimate=pl.CostEstimate(
            flops=2 * size * total * (members + chunk), bytes_accessed=6 * size * total, transcendentals=0),
        compiler_params=pltpu.CompilerParams(vmem_limit_bytes=24 << 20),
        name="final",
    )(where, transposed, *[block for _, block, _ in sides], left, right, *more)


def update_kernel(master_ref, right_ref, left_ref, new_ref):
    new_ref[...] = master_ref[...] + jnp.dot(right_ref[...], left_ref[...], preferred_element_type=jnp.float32)


def update(transposed, right, left):
    width, tile = transposed.shape
    members = right.shape[1]
    chunk = divisor(width, 16, 150)
    return pl.pallas_call(
        update_kernel,
        grid=(width // chunk,),
        in_specs=[
            pl.BlockSpec((chunk, tile), lambda i: (i, 0)),
            pl.BlockSpec((chunk, members), lambda i: (i, 0)),
            pl.BlockSpec((members, tile), lambda i: (0, 0)),
        ],
        out_specs=pl.BlockSpec((chunk, tile), lambda i: (i, 0)),
        out_shape=jax.ShapeDtypeStruct(transposed.shape, jnp.float32),
        cost_estimate=pl.CostEstimate(
            flops=2 * width * tile * members, bytes_accessed=8 * width * tile, transcendentals=0),
        compiler_params=pltpu.CompilerParams(vmem_limit_bytes=24 << 20),
        name="update",
    )(transposed, right, left)


def weigh_kernel(members, l_ref, r_ref, s_ref, w_ref, o_ref, t_ref, turned):
    answers, block = s_ref.shape[0] // members, s_ref.shape[2]
    population = members * block
    local = block // answers
    an = lax.axis_index("answer")
    scores = []
    for m in range(members):
        total = s_ref[m]
        for a in range(1, answers):
            total = total + s_ref[a * members + m]
        scores.append(total)
    average = sum(jnp.sum(x, axis=1, keepdims=True) for x in scores) / population
    squares = sum(jnp.sum(x * x, axis=1, keepdims=True) for x in scores) / population
    spread = jnp.sqrt(squares - average * average + 1e-05) * jnp.sqrt(jnp.float32(population))
    for m in range(members):
        scale = jnp.broadcast_to((scores[m] - average) / spread, (block, block)).T[:, :1]
        for a in range(answers):
            at = (a * members + m) * local
            rows = slice(at, at + local)
            w_ref[rows, :] = (l_ref[rows, :].astype(jnp.float32) * scale[a * local:(a + 1) * local]).astype(w_ref.dtype)
    rows = o_ref.shape[0]
    o_ref[...] = w_ref[:, pl.ds(pl.multiple_of(an * rows, 128), rows)].T
    turned[...] = r_ref[...].T
    width = t_ref.shape[0]
    t_ref[...] = turned[pl.ds(pl.multiple_of(an * width, 16), width), :]


def weigh(left_tile, right, parts, members, rows, width):
    vmem = pl.BlockSpec(memory_space=pltpu.VMEM)
    total = left_tile.shape[0]
    half = left_tile.dtype
    return pl.pallas_call(
        lambda *refs: weigh_kernel(members, *refs),
        out_shape=(
            jax.ShapeDtypeStruct(left_tile.shape, half),
            jax.ShapeDtypeStruct((rows, total), half),
            jax.ShapeDtypeStruct((width, total), half),
        ),
        in_specs=[vmem] * 3,
        out_specs=(vmem,) * 3,
        scratch_shapes=[pltpu.VMEM(right.shape[::-1], half)],
        cost_estimate=pl.CostEstimate(flops=total * right.shape[1] * 256, bytes_accessed=1 << 23, transcendentals=0),
        compiler_params=pltpu.CompilerParams(vmem_limit_bytes=24 << 20),
        name="weigh",
    )(left_tile, right, parts)


def split(rows):
    steps = rows // 128
    last = 1 if steps > 1 else 0
    first = (steps - last + 1) // 2
    return [n * 128 for n in (first, steps - last - first, last) if n]


def order_of(count):
    return [(c, x) for c in range(count) for x in (3, 2, 1)] + [(count - 1, 4)]


def fast_body(master, left_noise, right_noise, returns):
    members, answers = lax.axis_size("member"), lax.axis_size("answer")
    where = lax.axis_index("answer").astype(jnp.int32)[None]
    transposed = master.T
    width, tile = transposed.shape
    rows = tile // answers
    chunks = split(rows)
    last = len(chunks) - 1
    left_tile, right, parts, _, early, cross, aside, *blocks = exchange(left_noise, right_noise, returns, transposed, members, chunks)
    blocks = [blocks[i:i + len(chunks)] for i in range(0, len(blocks), len(chunks))]
    pairs = {1: [(0, 1), (1, 0), (2, 3), (3, 2)], 2: [(1, 3), (2, 0), (0, 2), (3, 1)], 3: [(0, 3), (3, 0)], 4: [(1, 2), (2, 1)]}
    got = {}
    for c, x in order_of(len(chunks)):
        some = {(last, 2): pairs[2][:2], (last, 1): pairs[1][::3]}.get((c, x), pairs[x])
        got[c, x] = lax.ppermute(blocks[min(x, 3) - 1][c], "answer", some)
    weighted, own, turned = weigh(left_tile, right, parts, members, rows, width)
    new_master = update(transposed, turned, weighted)
    rollout, at = None, 0
    for c, size in enumerate(chunks):
        sides = [((1, True if c == last else None), got[c, 1], 0), ((3, False), got[c, 3], 0)]
        if c == last:
            sides += [((1, False), aside, 0), ((2, True), cross, 0), ((2, False), got[c, 2], 0), ((3, True), got[c, 4], 0)]
        else:
            sides += [((2, None), got[c, 2], 0), ((3, True), early, at // 128)]
        rollout = finalize(where, transposed, sides, own, right, at, size, rollout)
        at += size
    return (new_master.T, rollout)


def fits(members, tensors, answers, tile, local):
    return (members, tensors, answers) == (2, 4, 4) and tile % 512 == 0 and tile >= 1024 and local % 32 == 0


def body(master, left_noise, right_noise, returns):
    sizes = [lax.axis_size(n) for n in ("member", "tensor", "answer")]
    fast = fits(*sizes, master.shape[0], left_noise.shape[0])
    return (fast_body if fast else plain_body)(master, left_noise, right_noise, returns)


def solution(mesh):
    return jax.shard_map(
        body,
        mesh=mesh,
        in_specs=(
            P("member", ("tensor", "answer")),
            P(("member", "answer"), None),
            P(("member", "answer"), "tensor"),
            P("member", "answer"),
        ),
        out_specs=(P("member", ("tensor", "answer")), P(("member", "answer"), "tensor")),
        check_vma=False,
    )
```

```python
import jax
import jax.numpy as jnp
from jax import lax
from jax.experimental import pallas as pl
from jax.experimental.pallas import tpu as pltpu
from jax.sharding import PartitionSpec as P


def contract(left_tile, accum, pieces):
    right_cols, weights = pieces
    weighted = left_tile.astype(jnp.float32) * weights[:, None]
    return accum + lax.dot_general(
        weighted,
        right_cols.astype(jnp.float32),
        (((0,), (0,)), ((), ())),
        precision=lax.Precision.HIGHEST,
    )


def plain_body(master, left_noise, right_noise, returns):
    member_count = lax.axis_size("member")
    answer_count = lax.axis_size("answer")
    partial_value = jnp.sum(returns, axis=1)
    block_len = partial_value.shape[0]
    population = block_len * member_count
    scores = lax.psum(partial_value, "answer")
    score_sum, square_sum = lax.psum((jnp.sum(scores), jnp.sum(scores * scores)), "member")
    average = score_sum / population
    variance = square_sum / population - average * average
    fitness = (scores - average) / jnp.sqrt(variance + 1e-05)
    tile_rows = master.shape[0]
    local_members = left_noise.shape[0]
    restricted = lax.all_to_all(left_noise, "member", split_axis=1, concat_axis=0, tiled=True)
    gathered_rows = lax.all_gather(restricted, "answer", axis=0, tiled=True)
    width = gathered_rows.shape[1]
    left_tile = gathered_rows.reshape(answer_count, member_count, local_members, width)
    left_tile = jnp.transpose(left_tile, (1, 0, 2, 3)).reshape(
        answer_count * member_count * local_members, width
    )
    right_block = lax.all_to_all(right_noise, "answer", split_axis=1, concat_axis=0, tiled=True)
    initial = jnp.zeros((tile_rows, right_block.shape[1]), jnp.float32)
    update = contract(
        left_tile,
        initial,
        (
            lax.all_gather(right_block, "member", axis=0, tiled=True),
            lax.all_gather(fitness.astype(jnp.bfloat16), "member", axis=0, tiled=True).astype(
                jnp.float32
            ),
        ),
    )
    new_master = master + update / jnp.sqrt(jnp.float32(population))
    rollout = lax.all_to_all(
        new_master.astype(jnp.bfloat16), "answer", split_axis=0, concat_axis=1, tiled=True
    )
    return (new_master, rollout)


def exchange_kernel(members, chunks, left_hbm, right_hbm, returns_hbm, master_ref, *refs):
    sides = 3
    l_ref, r_ref, s_ref, p_ref, e_ref, n_ref, b_ref, *refs = refs
    blocks, refs = refs[:sides * len(chunks)], refs[sides * len(chunks):]
    (left_ref, right_ref, returns_ref, load_sem, wide, narrow, part, own_sem, pull_sem, push_sem, s_send, s_recv, t_send, t_recv, x_send, x_recv, f_send, f_recv,
     z_send, z_recv, q_send, q_recv, y_send, y_recv, e_send, e_recv, n_send, n_recv, b_send, b_recv) = refs
    me, te, an = lax.axis_index("member"), lax.axis_index("tensor"), lax.axis_index("answer")
    answers = 4
    local = left_ref.shape[0]
    slab = local * members
    tile = l_ref.shape[1]
    piece = tile // 4
    rows = tile // answers
    beside = lambda i: i + 1 - 2 * lax.rem(i, 2)
    other, core, across = 1 - me, beside(te), lax.rem(te + 2, 4)
    near, far = beside(an), 2 - lax.div(an, 2)
    beyond = 2 * (1 - lax.div(an, 2))
    inner = lax.div(an + 1, 2) == 1
    outer = jnp.logical_not(inner)
    pair = {1: near, 2: lax.rem(an + 2, answers), 3: answers - 1 - an}

    def l_at(start, count, t):
        return l_ref.at[pl.ds(pl.multiple_of(start, local), count), pl.ds(pl.multiple_of(t * piece, piece), piece)]

    def l_slab(a, t):
        return l_at(a * slab, slab, t)

    def r_at(a, m):
        return r_ref.at[pl.ds(pl.multiple_of((a * members + m) * local, local), local), :]

    def remote(src, dst, send, recv, where):
        return pltpu.make_async_remote_copy(src_ref=src, dst_ref=dst, send_sem=send, recv_sem=recv,
                                            device_id=where, device_id_type=pl.DeviceIdType.MESH)

    def pull(x):
        return pltpu.make_async_copy(
            master_ref.at[:, pl.ds(pl.multiple_of(pair[x] * rows, rows), rows)], wide.at[x % 2], pull_sem.at[x - 1])

    def push(x, c):
        at = sum(chunks[:c])
        return pltpu.make_async_copy(
            narrow.at[x % 2, :, at:at + chunks[c]], blocks[(x - 1) * len(chunks) + c], push_sem.at[x - 1, c])

    def cast(x):
        pull(x).wait()
        step = 96

        def one(i, _):
            at = pl.ds(pl.multiple_of(i * step, step), step)
            narrow[x % 2, at, :] = wide[x % 2, at, :].astype(narrow.dtype)
            return 0

        lax.fori_loop(0, narrow.shape[1] // step, one, 0)
        for c in range(len(chunks)):
            push(x, c).start()

    barrier = pltpu.get_barrier_semaphore()

    def greet(where):
        pl.semaphore_signal(barrier, inc=1, device_id=where, device_id_type=pl.DeviceIdType.MESH)

    for where in ({"answer": near}, {"member": other}, {"tensor": core}, {"tensor": across}):
        greet(where)

    @pl.when(inner)
    def _():
        greet({"answer": beyond})
        greet({"answer": beyond + 1})

    loads = [pltpu.make_async_copy(src, dst, load_sem.at[i]) for i, (src, dst) in enumerate(
        ((right_hbm, right_ref), (left_hbm, left_ref), (returns_hbm, returns_ref)))]
    for load in loads:
        load.start()
    pull(1).start()
    pull(2).start()
    loads[0].wait()
    own_r = pltpu.make_async_copy(right_ref, r_at(an, me), own_sem.at[1])
    own_r.start()
    pl.semaphore_wait(barrier, 5)

    mine = lax.rem(an, 2)
    halves = 2
    count = local // halves
    sources = (an, near, beyond, beyond + 1)
    started = []

    def start(copy):
        copy.start()
        started.append(copy)
        return copy

    def landed(block, sem):
        remote(block, block, x_send.at[0], sem, {"member": other}).wait_recv()

    def r_half(a, m, h):
        return r_ref.at[pl.ds(pl.multiple_of((a * members + m) * local + h * count, count), count), :]

    def forward(k, h):
        block = r_half(sources[k], me, h)
        src = right_ref.at[h * count:(h + 1) * count, :] if k == 0 else block
        start(remote(src, block, f_send.at[k, h], f_recv.at[k, h], {"member": other}))

    def spread(k):
        block = l_slab(sources[k], te)
        start(remote(block, block, y_send.at[k, 0], y_recv.at[k, 0], {"tensor": across}))
        start(remote(block, block, y_send.at[k, 1], y_recv.at[k, 1], {"tensor": core}))

    def part_of(h):
        src = right_ref.at[h * count:(h + 1) * count, :]
        start(remote(src, r_half(an, me, h), z_send.at[0, h], z_recv.at[1 + mine, h], {"answer": far}))
        start(remote(src, r_half(an, me, h), z_send.at[1, h], z_recv.at[0, h], {"answer": near}))

    part_of(0)
    loads[1].wait()
    start(remote(left_ref.at[:, pl.ds(pl.multiple_of(other * tile + te * piece, piece), piece)],
                 l_at((an * members + me) * local, local, te), x_send.at[0], x_recv.at[0], {"member": other}))
    own_l = pltpu.make_async_copy(
        left_ref.at[:, pl.ds(pl.multiple_of(me * tile + te * piece, piece), piece)],
        l_at((an * members + me) * local, local, te), own_sem.at[0])
    own_l.start()
    loads[2].wait()
    part[...] = jnp.sum(returns_ref[...].T, axis=0, keepdims=True)
    own_p = pltpu.make_async_copy(part, p_ref, own_sem.at[2])
    own_s = pltpu.make_async_copy(part, s_ref.at[an * members + me], own_sem.at[3])
    own_p.start()
    own_s.start()
    own_p.wait()
    score = lambda a, m: s_ref.at[a * members + m]
    start(remote(p_ref, score(an, me), s_send.at[0], s_recv.at[mine + 1], {"answer": far}))
    start(remote(p_ref, score(an, me), s_send.at[1], s_recv.at[0], {"answer": near}))
    start(remote(p_ref, score(an, me), t_send.at[0], t_recv.at[0], {"member": other}))
    own_l.wait()
    landed(l_at((an * members + other) * local, local, te), x_recv.at[0])
    block = l_slab(an, te)
    start(remote(block, block, q_send.at[0], q_recv.at[1 + mine], {"answer": far}))
    start(remote(block, block, q_send.at[1], q_recv.at[0], {"answer": near}))
    part_of(1)
    spread(0)
    for h in range(halves):
        forward(0, h)
    last = len(chunks) - 1
    cast(1)
    push(1, last).wait()
    aside = remote(blocks[last], b_ref, b_send, b_recv, {"answer": near})
    pl.when(inner)(aside.start)
    for c in range(last):
        push(1, c).wait()
    pull(3).start()
    cast(2)
    push(2, last).wait()
    cross = remote(blocks[len(chunks) + last], n_ref, n_send, n_recv, {"answer": far})
    pl.when(outer)(cross.start)
    cast(3)
    early = []
    push(3, last).wait()
    for c, size in enumerate(chunks[:last]):
        push(3, c).wait()
        at = sum(chunks[:c])
        copy = remote(blocks[2 * len(chunks) + c], e_ref.at[:, at:at + size], e_send.at[c], e_recv.at[c], {"answer": pair[3]})
        pl.when(inner)(copy.start)
        early.append(copy)
    for h in range(halves):
        landed(r_half(near, me, h), z_recv.at[0, h])
        forward(1, h)
    landed(l_slab(near, te), q_recv.at[0])
    spread(1)
    relays = []

    def relay(block, send, recv):
        copy = remote(block, block, send, recv, {"answer": near})
        pl.when(inner)(copy.start)
        relays.append(copy)

    def pass_on(h):
        for k in (2, 3):
            block = r_half(sources[k], me, h)
            landed(block, z_recv.at[k - 1, h])
            relay(block, z_send.at[k, h], z_recv.at[k - 1, h])
            forward(k, h)

    pass_on(0)
    for k in (2, 3):
        block = l_slab(sources[k], te)
        landed(block, q_recv.at[k - 1])
        relay(block, q_send.at[k], q_recv.at[k - 1])
        spread(k)
    pass_on(1)
    for k in range(answers):
        block = l_slab(sources[k], across)
        landed(block, y_recv.at[k, 0])
        start(remote(block, block, y_send.at[k, 2], y_recv.at[k, 2], {"tensor": core}))
    for k in range(1, answers):
        block = score(sources[k], me)
        landed(block, s_recv.at[k - 1])
        if k > 1:
            relay(block, s_send.at[k], s_recv.at[k - 1])
        start(remote(block, block, t_send.at[k], t_recv.at[k], {"member": other}))
    for k in range(answers):
        landed(score(sources[k], other), t_recv.at[k])
    for k in range(answers):
        for h in range(halves):
            landed(r_half(sources[k], other, h), f_recv.at[k, h])
    for k in range(answers):
        landed(l_slab(sources[k], core), y_recv.at[k, 1])
        landed(l_slab(sources[k], 3 - te), y_recv.at[k, 2])
    own_r.wait()
    own_s.wait()
    for c in range(last):
        push(2, c).wait()
    for copy in started:
        copy.wait_send()
    for copy in relays + early:
        pl.when(inner)(copy.wait_send)
    for copy in early:
        pl.when(inner)(copy.wait_recv)
    pl.when(outer)(cross.wait_send)
    pl.when(inner)(cross.wait_recv)
    pl.when(inner)(aside.wait_send)
    pl.when(outer)(aside.wait_recv)


def exchange(left_noise, right_noise, returns, transposed, members, chunks):
    answers, sides = 4, 3
    local, width = right_noise.shape
    cols, tile = transposed.shape
    total = local * members * answers
    count = members * answers
    block = returns.shape[0]
    half = left_noise.dtype
    dma = pltpu.SemaphoreType.DMA
    anywhere = pl.BlockSpec(memory_space=pl.ANY)
    shape = jax.ShapeDtypeStruct
    return pl.pallas_call(
        lambda *refs: exchange_kernel(members, chunks, *refs),
        out_shape=(
            shape((total, tile), half),
            shape((total, width), half),
            shape((count, 1, block), jnp.float32),
            shape((1, block), jnp.float32),
            shape((cols, sum(chunks[:-1])), half),
            shape((cols, chunks[-1]), half),
            shape((cols, chunks[-1]), half),
        ) + tuple(shape((cols, size), half) for _ in range(sides) for size in chunks),
        in_specs=[anywhere] * 4,
        out_specs=(anywhere,) * (7 + sides * len(chunks)),
        scratch_shapes=[
            pltpu.VMEM(left_noise.shape, half), pltpu.VMEM(right_noise.shape, half),
            pltpu.VMEM(returns.shape, returns.dtype), dma((3,)),
            pltpu.VMEM((2, cols, tile // answers), jnp.float32), pltpu.VMEM((2, cols, tile // answers), half),
            pltpu.VMEM((1, block), jnp.float32),
            dma((4,)), dma((sides,)), dma((sides, len(chunks))), dma((4,)), dma((3,)), dma((4,)), dma((4,)),
            dma((1,)), dma((1,)), dma((answers, 2)), dma((answers, 2)),
            dma((4, 2)), dma((3, 2)), dma((4,)), dma((3,)), dma((answers, 3)), dma((answers, 3)),
            dma((len(chunks) - 1,)), dma((len(chunks) - 1,)), dma, dma, dma, dma,
        ],
        compiler_params=pltpu.CompilerParams(collective_id=0, has_side_effects=True),
        name="exchange",
    )(left_noise, right_noise, returns, transposed)


def divisor(size, least, most):
    fits = [n for n in range(least, most + 1, least) if size % n == 0]
    return fits[-1] if fits else size


def final_kernel(picks, where_ref, master_ref, *refs):
    sides, refs = refs[:len(picks)], refs[len(picks):]
    left_ref, right_ref, out_ref, stack = refs[0], refs[1], refs[-2], refs[-1]
    an = lax.axis_index("answer")
    width, rows = master_ref.shape
    near = an + 1 - 2 * lax.rem(an, 2)
    inner = lax.div(an + 1, 2) == 1
    places = {1: near, 2: lax.rem(an + 2, 4), 3: 3 - an}
    within = {True: inner, False: jnp.logical_not(inner)}

    def place(a, ref):
        stack[pl.ds(pl.multiple_of(a * width, 16), width), :] = ref[...].astype(stack.dtype)

    place(an, master_ref)
    for (x, which), ref in zip(picks, sides):
        if which is None:
            place(places[x], ref)
        else:
            pl.when(within[which])(lambda x=x, ref=ref: place(places[x], ref))
    row = lax.broadcasted_iota(jnp.int32, (rows, rows), 0)
    col = lax.broadcasted_iota(jnp.int32, (rows, rows), 1)
    unit = jnp.where(row == col, 1.0, 0.0).astype(stack.dtype)
    step = divisor(out_ref.shape[1], 128, 512)
    for at in range(0, out_ref.shape[1], step):
        cols = slice(at, at + step)
        new = jnp.dot(left_ref[...], right_ref[:, cols], preferred_element_type=jnp.float32)
        old = lax.dot_general(unit, stack[cols, :], (((1,), (1,)), ((), ())), preferred_element_type=jnp.float32)
        out_ref[:, cols] = (new + old).astype(out_ref.dtype)


def finalize(where, transposed, sides, left, right, first, size, so_far):
    rows, members = left.shape
    width = transposed.shape[0]
    total = right.shape[1]
    chunk = 128
    start, steps = first // chunk, size // chunk
    per = rows // chunk
    more = [] if so_far is None else [so_far]
    picks = tuple(key for key, _, _ in sides)
    blocks = [pl.BlockSpec((width, chunk), lambda i, w, at=at: (0, at + i)) for _, _, at in sides]
    return pl.pallas_call(
        lambda *refs: final_kernel(picks, *refs),
        grid_spec=pltpu.PrefetchScalarGridSpec(
            num_scalar_prefetch=1,
            grid=(steps,),
            in_specs=[pl.BlockSpec((width, chunk), lambda i, w: (0, w[0] * per + start + i))] + blocks + [
                pl.BlockSpec((chunk, members), lambda i, w: (start + i, 0)),
                pl.BlockSpec((members, total), lambda i, w: (0, 0)),
            ] + [pl.BlockSpec(memory_space=pl.ANY)] * len(more),
            out_specs=pl.BlockSpec((chunk, total), lambda i, w: (start + i, 0)),
            scratch_shapes=[pltpu.VMEM((total, chunk), jnp.bfloat16)],
        ),
        out_shape=jax.ShapeDtypeStruct((rows, total), jnp.bfloat16),
        input_output_aliases={4 + len(sides): 0} if more else {},
        cost_estimate=pl.CostEstimate(
            flops=2 * size * total * (members + chunk), bytes_accessed=6 * size * total, transcendentals=0),
        compiler_params=pltpu.CompilerParams(vmem_limit_bytes=24 << 20),
        name="final",
    )(where, transposed, *[block for _, block, _ in sides], left, right, *more)


def last_kernel(picks, first, master_ref, *refs):
    sides, refs = refs[:len(picks)], refs[len(picks):]
    base_ref, _, out_ref, stack, block, sem = refs
    an = lax.axis_index("answer")
    width, tile = master_ref.shape
    rows = block.shape[0]
    places = {0: an, 1: an + 1 - 2 * lax.rem(an, 2), 2: lax.rem(an + 2, 4), 3: 3 - an}
    inner = lax.div(an + 1, 2) == 1
    within = {True: inner, False: jnp.logical_not(inner)}

    def place(x, value):
        stack[pl.ds(pl.multiple_of(places[x] * width, 16), width), :] = value.astype(stack.dtype)

    place(0, master_ref[:, pl.ds(pl.multiple_of(an * (tile // 4) + first, 128), rows)])
    for (x, which), ref in zip(picks, sides):
        pl.when(within[which])(lambda x=x, ref=ref: place(x, ref[...]))
    row = lax.broadcasted_iota(jnp.int32, (rows, rows), 0)
    col = lax.broadcasted_iota(jnp.int32, (rows, rows), 1)
    unit = jnp.where(row == col, 1.0, 0.0).astype(stack.dtype)
    total = out_ref.shape[1]
    step = divisor(total, 128, 512)
    copies = []
    for i, at in enumerate(range(0, total, step)):
        cols = slice(at, at + step)
        old = lax.dot_general(unit, stack[cols, :], (((1,), (1,)), ((), ())), preferred_element_type=jnp.float32)
        block[:, cols] = (base_ref[:, cols] + old).astype(block.dtype)
        copy = pltpu.make_async_copy(block.at[:, cols], out_ref.at[first:first + rows, cols], sem.at[i])
        copy.start()
        copies.append(copy)
    for copy in copies:
        copy.wait()


def finish(transposed, sides, base, first, so_far):
    size, total = base.shape
    vmem, anywhere = pl.BlockSpec(memory_space=pltpu.VMEM), pl.BlockSpec(memory_space=pl.ANY)
    picks = tuple(key for key, _, _ in sides)
    return pl.pallas_call(
        lambda *refs: last_kernel(picks, first, *refs),
        in_specs=[vmem] * (2 + len(sides)) + [anywhere],
        out_specs=anywhere,
        scratch_shapes=[
            pltpu.VMEM((total, size), so_far.dtype), pltpu.VMEM((size, total), so_far.dtype),
            pltpu.SemaphoreType.DMA((total // divisor(total, 128, 512),)),
        ],
        out_shape=jax.ShapeDtypeStruct(so_far.shape, so_far.dtype),
        input_output_aliases={2 + len(sides): 0},
        cost_estimate=pl.CostEstimate(
            flops=2 * size * total * size, bytes_accessed=6 * size * total, transcendentals=0),
        compiler_params=pltpu.CompilerParams(vmem_limit_bytes=24 << 20),
        name="last",
    )(transposed, *[block for _, block, _ in sides], base, so_far)


def update_kernel(master_ref, right_ref, left_ref, new_ref):
    new_ref[...] = master_ref[...] + jnp.dot(right_ref[...], left_ref[...], preferred_element_type=jnp.float32)


def update(transposed, right, left):
    width, tile = transposed.shape
    members = right.shape[1]
    chunk = divisor(width, 16, 150)
    return pl.pallas_call(
        update_kernel,
        grid=(width // chunk,),
        in_specs=[
            pl.BlockSpec((chunk, tile), lambda i: (i, 0)),
            pl.BlockSpec((chunk, members), lambda i: (i, 0)),
            pl.BlockSpec((members, tile), lambda i: (0, 0)),
        ],
        out_specs=pl.BlockSpec((chunk, tile), lambda i: (i, 0)),
        out_shape=jax.ShapeDtypeStruct(transposed.shape, jnp.float32),
        cost_estimate=pl.CostEstimate(
            flops=2 * width * tile * members, bytes_accessed=8 * width * tile, transcendentals=0),
        compiler_params=pltpu.CompilerParams(vmem_limit_bytes=24 << 20),
        name="update",
    )(transposed, right, left)


def weigh_kernel(members, l_ref, r_ref, s_ref, w_ref, o_ref, t_ref, b_ref, turned):
    answers, block = s_ref.shape[0] // members, s_ref.shape[2]
    population = members * block
    local = block // answers
    an = lax.axis_index("answer")
    scores = []
    for m in range(members):
        total = s_ref[m]
        for a in range(1, answers):
            total = total + s_ref[a * members + m]
        scores.append(total)
    average = sum(jnp.sum(x, axis=1, keepdims=True) for x in scores) / population
    squares = sum(jnp.sum(x * x, axis=1, keepdims=True) for x in scores) / population
    spread = jnp.sqrt(squares - average * average + 1e-05) * jnp.sqrt(jnp.float32(population))
    for m in range(members):
        scale = jnp.broadcast_to((scores[m] - average) / spread, (block, block)).T[:, :1]
        for a in range(answers):
            at = (a * members + m) * local
            rows = slice(at, at + local)
            w_ref[rows, :] = (l_ref[rows, :].astype(jnp.float32) * scale[a * local:(a + 1) * local]).astype(w_ref.dtype)
    rows = o_ref.shape[0]
    o_ref[...] = w_ref[:, pl.ds(pl.multiple_of(an * rows, 128), rows)].T
    turned[...] = r_ref[...].T
    width = t_ref.shape[0]
    t_ref[...] = turned[pl.ds(pl.multiple_of(an * width, 16), width), :]
    step = divisor(b_ref.shape[1], 128, 512)
    for at in range(0, b_ref.shape[1], step):
        b_ref[:, at:at + step] = jnp.dot(
            o_ref[rows - b_ref.shape[0]:, :], r_ref[:, at:at + step], preferred_element_type=jnp.float32)


def weigh(left_tile, right, parts, members, rows, width, size):
    vmem = pl.BlockSpec(memory_space=pltpu.VMEM)
    total = left_tile.shape[0]
    half = left_tile.dtype
    return pl.pallas_call(
        lambda *refs: weigh_kernel(members, *refs),
        out_shape=(
            jax.ShapeDtypeStruct(left_tile.shape, half),
            jax.ShapeDtypeStruct((rows, total), half),
            jax.ShapeDtypeStruct((width, total), half),
            jax.ShapeDtypeStruct((size, right.shape[1]), jnp.float32),
        ),
        in_specs=[vmem] * 3,
        out_specs=(vmem,) * 4,
        scratch_shapes=[pltpu.VMEM(right.shape[::-1], half)],
        cost_estimate=pl.CostEstimate(flops=total * right.shape[1] * 256, bytes_accessed=1 << 23, transcendentals=0),
        compiler_params=pltpu.CompilerParams(vmem_limit_bytes=24 << 20),
        name="weigh",
    )(left_tile, right, parts)


def split(rows):
    steps = rows // 128
    last = 1 if steps > 1 else 0
    first = (steps - last + 1) // 2
    return [n * 128 for n in (first, steps - last - first, last) if n]


def order_of(count):
    return [(c, x) for c in range(count) for x in (3, 2, 1)] + [(count - 1, 4)]


def fast_body(master, left_noise, right_noise, returns):
    members, answers = lax.axis_size("member"), lax.axis_size("answer")
    where = lax.axis_index("answer").astype(jnp.int32)[None]
    transposed = master.T
    width, tile = transposed.shape
    rows = tile // answers
    chunks = split(rows)
    last = len(chunks) - 1
    left_tile, right, parts, _, early, cross, aside, *blocks = exchange(left_noise, right_noise, returns, transposed, members, chunks)
    blocks = [blocks[i:i + len(chunks)] for i in range(0, len(blocks), len(chunks))]
    pairs = {1: [(0, 1), (1, 0), (2, 3), (3, 2)], 2: [(1, 3), (2, 0), (0, 2), (3, 1)], 3: [(0, 3), (3, 0)], 4: [(1, 2), (2, 1)]}
    got = {}
    for c, x in order_of(len(chunks)):
        some = {(last, 2): pairs[2][:2], (last, 1): pairs[1][::3]}.get((c, x), pairs[x])
        got[c, x] = lax.ppermute(blocks[min(x, 3) - 1][c], "answer", some)
    weighted, own, turned, base = weigh(left_tile, right, parts, members, rows, width, chunks[-1])
    new_master = update(transposed, turned, weighted)
    rollout, at = None, 0
    for c, size in enumerate(chunks):
        sides = [((1, True if c == last else None), got[c, 1], 0), ((3, False), got[c, 3], 0)]
        if c == last:
            sides += [((1, False), aside, 0), ((2, True), cross, 0), ((2, False), got[c, 2], 0), ((3, True), got[c, 4], 0)]
        else:
            sides += [((2, None), got[c, 2], 0), ((3, True), early, at // 128)]
        if c == last:
            rollout = finish(transposed, sides, base, at, rollout)
        else:
            rollout = finalize(where, transposed, sides, own, right, at, size, rollout)
        at += size
    return (new_master.T, rollout)


def fits(members, tensors, answers, tile, local):
    return (members, tensors, answers) == (2, 4, 4) and tile % 512 == 0 and tile >= 1024 and local % 32 == 0


def body(master, left_noise, right_noise, returns):
    sizes = [lax.axis_size(n) for n in ("member", "tensor", "answer")]
    fast = fits(*sizes, master.shape[0], left_noise.shape[0])
    return (fast_body if fast else plain_body)(master, left_noise, right_noise, returns)


def solution(mesh):
    return jax.shard_map(
        body,
        mesh=mesh,
        in_specs=(
            P("member", ("tensor", "answer")),
            P(("member", "answer"), None),
            P(("member", "answer"), "tensor"),
            P("member", "answer"),
        ),
        out_specs=(P("member", ("tensor", "answer")), P(("member", "answer"), "tensor")),
        check_vma=False,
    )
```

```python
import jax
import jax.numpy as jnp
from jax import lax
from jax.experimental import pallas as pl
from jax.experimental.pallas import tpu as pltpu
from jax.sharding import PartitionSpec as P


def contract(left_tile, accum, pieces):
    right_cols, weights = pieces
    weighted = left_tile.astype(jnp.float32) * weights[:, None]
    return accum + lax.dot_general(
        weighted,
        right_cols.astype(jnp.float32),
        (((0,), (0,)), ((), ())),
        precision=lax.Precision.HIGHEST,
    )


def plain_body(master, left_noise, right_noise, returns):
    member_count = lax.axis_size("member")
    answer_count = lax.axis_size("answer")
    partial_value = jnp.sum(returns, axis=1)
    block_len = partial_value.shape[0]
    population = block_len * member_count
    scores = lax.psum(partial_value, "answer")
    score_sum, square_sum = lax.psum((jnp.sum(scores), jnp.sum(scores * scores)), "member")
    average = score_sum / population
    variance = square_sum / population - average * average
    fitness = (scores - average) / jnp.sqrt(variance + 1e-05)
    tile_rows = master.shape[0]
    local_members = left_noise.shape[0]
    restricted = lax.all_to_all(left_noise, "member", split_axis=1, concat_axis=0, tiled=True)
    gathered_rows = lax.all_gather(restricted, "answer", axis=0, tiled=True)
    width = gathered_rows.shape[1]
    left_tile = gathered_rows.reshape(answer_count, member_count, local_members, width)
    left_tile = jnp.transpose(left_tile, (1, 0, 2, 3)).reshape(
        answer_count * member_count * local_members, width
    )
    right_block = lax.all_to_all(right_noise, "answer", split_axis=1, concat_axis=0, tiled=True)
    initial = jnp.zeros((tile_rows, right_block.shape[1]), jnp.float32)
    update = contract(
        left_tile,
        initial,
        (
            lax.all_gather(right_block, "member", axis=0, tiled=True),
            lax.all_gather(fitness.astype(jnp.bfloat16), "member", axis=0, tiled=True).astype(
                jnp.float32
            ),
        ),
    )
    new_master = master + update / jnp.sqrt(jnp.float32(population))
    rollout = lax.all_to_all(
        new_master.astype(jnp.bfloat16), "answer", split_axis=0, concat_axis=1, tiled=True
    )
    return (new_master, rollout)


def exchange_kernel(members, chunks, left_hbm, right_hbm, returns_hbm, master_ref, *refs):
    sides = 3
    l_ref, r_ref, s_ref, p_ref, e_ref, n_ref, b_ref, *refs = refs
    blocks, refs = refs[:sides * len(chunks)], refs[sides * len(chunks):]
    (left_ref, right_ref, returns_ref, load_sem, wide, narrow, part, own_sem, pull_sem, push_sem, s_send, s_recv, t_send, t_recv, x_send, x_recv, f_send, f_recv,
     z_send, z_recv, q_send, q_recv, y_send, y_recv, e_send, e_recv, n_send, n_recv, b_send, b_recv) = refs
    me, te, an = lax.axis_index("member"), lax.axis_index("tensor"), lax.axis_index("answer")
    answers = 4
    local = left_ref.shape[0]
    slab = local * members
    tile = l_ref.shape[1]
    piece = tile // 4
    rows = tile // answers
    beside = lambda i: i + 1 - 2 * lax.rem(i, 2)
    other, core, across = 1 - me, beside(te), lax.rem(te + 2, 4)
    near, far = beside(an), 2 - lax.div(an, 2)
    beyond = 2 * (1 - lax.div(an, 2))
    inner = lax.div(an + 1, 2) == 1
    outer = jnp.logical_not(inner)
    pair = {1: near, 2: lax.rem(an + 2, answers), 3: answers - 1 - an}

    def l_at(start, count, t):
        return l_ref.at[pl.ds(pl.multiple_of(start, local), count), pl.ds(pl.multiple_of(t * piece, piece), piece)]

    def l_slab(a, t):
        return l_at(a * slab, slab, t)

    def r_at(a, m):
        return r_ref.at[pl.ds(pl.multiple_of((a * members + m) * local, local), local), :]

    def remote(src, dst, send, recv, where):
        return pltpu.make_async_remote_copy(src_ref=src, dst_ref=dst, send_sem=send, recv_sem=recv,
                                            device_id=where, device_id_type=pl.DeviceIdType.MESH)

    def pull(x):
        return pltpu.make_async_copy(
            master_ref.at[:, pl.ds(pl.multiple_of(pair[x] * rows, rows), rows)], wide.at[x % 2], pull_sem.at[x - 1])

    def push(x, c):
        at = sum(chunks[:c])
        return pltpu.make_async_copy(
            narrow.at[x % 2, :, at:at + chunks[c]], blocks[(x - 1) * len(chunks) + c], push_sem.at[x - 1, c])

    def cast(x):
        pull(x).wait()
        step = 96

        def one(i, _):
            at = pl.ds(pl.multiple_of(i * step, step), step)
            narrow[x % 2, at, :] = wide[x % 2, at, :].astype(narrow.dtype)
            return 0

        lax.fori_loop(0, narrow.shape[1] // step, one, 0)
        for c in range(len(chunks)):
            push(x, c).start()

    barrier = pltpu.get_barrier_semaphore()

    def greet(where):
        pl.semaphore_signal(barrier, inc=1, device_id=where, device_id_type=pl.DeviceIdType.MESH)

    for where in ({"answer": near}, {"member": other}, {"tensor": core}, {"tensor": across}):
        greet(where)

    @pl.when(inner)
    def _():
        greet({"answer": beyond})
        greet({"answer": beyond + 1})

    loads = [pltpu.make_async_copy(src, dst, load_sem.at[i]) for i, (src, dst) in enumerate(
        ((right_hbm, right_ref), (left_hbm, left_ref), (returns_hbm, returns_ref)))]
    for load in loads:
        load.start()
    pull(1).start()
    pull(2).start()
    loads[0].wait()
    own_r = pltpu.make_async_copy(right_ref, r_at(an, me), own_sem.at[1])
    own_r.start()
    pl.semaphore_wait(barrier, 5)

    mine = lax.rem(an, 2)
    halves = 2
    count = local // halves
    sources = (an, near, beyond, beyond + 1)
    started = []

    def start(copy):
        copy.start()
        started.append(copy)
        return copy

    def landed(block, sem):
        remote(block, block, x_send.at[0], sem, {"member": other}).wait_recv()

    def r_half(a, m, h):
        return r_ref.at[pl.ds(pl.multiple_of((a * members + m) * local + h * count, count), count), :]

    def forward(k, h):
        block = r_half(sources[k], me, h)
        src = right_ref.at[h * count:(h + 1) * count, :] if k == 0 else block
        start(remote(src, block, f_send.at[k, h], f_recv.at[k, h], {"member": other}))

    def spread(k):
        block = l_slab(sources[k], te)
        start(remote(block, block, y_send.at[k, 0], y_recv.at[k, 0], {"tensor": across}))
        start(remote(block, block, y_send.at[k, 1], y_recv.at[k, 1], {"tensor": core}))

    def part_of(h):
        src = right_ref.at[h * count:(h + 1) * count, :]
        start(remote(src, r_half(an, me, h), z_send.at[0, h], z_recv.at[1 + mine, h], {"answer": far}))
        start(remote(src, r_half(an, me, h), z_send.at[1, h], z_recv.at[0, h], {"answer": near}))

    part_of(0)
    loads[1].wait()
    start(remote(left_ref.at[:, pl.ds(pl.multiple_of(other * tile + te * piece, piece), piece)],
                 l_at((an * members + me) * local, local, te), x_send.at[0], x_recv.at[0], {"member": other}))
    own_l = pltpu.make_async_copy(
        left_ref.at[:, pl.ds(pl.multiple_of(me * tile + te * piece, piece), piece)],
        l_at((an * members + me) * local, local, te), own_sem.at[0])
    own_l.start()
    loads[2].wait()
    part[...] = jnp.sum(returns_ref[...].T, axis=0, keepdims=True)
    own_p = pltpu.make_async_copy(part, p_ref, own_sem.at[2])
    own_s = pltpu.make_async_copy(part, s_ref.at[an * members + me], own_sem.at[3])
    own_p.start()
    own_s.start()
    own_p.wait()
    score = lambda a, m: s_ref.at[a * members + m]
    start(remote(p_ref, score(an, me), s_send.at[0], s_recv.at[mine + 1], {"answer": far}))
    start(remote(p_ref, score(an, me), s_send.at[1], s_recv.at[0], {"answer": near}))
    start(remote(p_ref, score(an, me), t_send.at[0], t_recv.at[0], {"member": other}))
    own_l.wait()
    landed(l_at((an * members + other) * local, local, te), x_recv.at[0])
    block = l_slab(an, te)
    start(remote(block, block, q_send.at[0], q_recv.at[1 + mine], {"answer": far}))
    start(remote(block, block, q_send.at[1], q_recv.at[0], {"answer": near}))
    part_of(1)
    spread(0)
    for h in range(halves):
        forward(0, h)
    last = len(chunks) - 1
    cast(1)
    push(1, last).wait()
    aside = remote(blocks[last], b_ref, b_send, b_recv, {"answer": near})
    pl.when(inner)(aside.start)
    for c in range(last):
        push(1, c).wait()
    pull(3).start()
    cast(2)
    push(2, last).wait()
    cross = remote(blocks[len(chunks) + last], n_ref, n_send, n_recv, {"answer": far})
    pl.when(outer)(cross.start)
    cast(3)
    early = []
    push(3, last).wait()
    for c, size in enumerate(chunks[:last]):
        push(3, c).wait()
        at = sum(chunks[:c])
        copy = remote(blocks[2 * len(chunks) + c], e_ref.at[:, at:at + size], e_send.at[c], e_recv.at[c], {"answer": pair[3]})
        pl.when(inner)(copy.start)
        early.append(copy)
    for h in range(halves):
        landed(r_half(near, me, h), z_recv.at[0, h])
        forward(1, h)
    landed(l_slab(near, te), q_recv.at[0])
    spread(1)
    relays = []

    def relay(block, send, recv):
        copy = remote(block, block, send, recv, {"answer": near})
        pl.when(inner)(copy.start)
        relays.append(copy)

    def pass_on(h):
        for k in (2, 3):
            block = r_half(sources[k], me, h)
            landed(block, z_recv.at[k - 1, h])
            relay(block, z_send.at[k, h], z_recv.at[k - 1, h])
            forward(k, h)

    pass_on(0)
    for k in (2, 3):
        block = l_slab(sources[k], te)
        landed(block, q_recv.at[k - 1])
        relay(block, q_send.at[k], q_recv.at[k - 1])
        spread(k)
    pass_on(1)
    for k in range(answers):
        block = l_slab(sources[k], across)
        landed(block, y_recv.at[k, 0])
        start(remote(block, block, y_send.at[k, 2], y_recv.at[k, 2], {"tensor": core}))
    for k in range(1, answers):
        block = score(sources[k], me)
        landed(block, s_recv.at[k - 1])
        if k > 1:
            relay(block, s_send.at[k], s_recv.at[k - 1])
        start(remote(block, block, t_send.at[k], t_recv.at[k], {"member": other}))
    for k in range(answers):
        landed(score(sources[k], other), t_recv.at[k])
    for k in range(answers):
        for h in range(halves):
            landed(r_half(sources[k], other, h), f_recv.at[k, h])
    for k in range(answers):
        landed(l_slab(sources[k], core), y_recv.at[k, 1])
        landed(l_slab(sources[k], 3 - te), y_recv.at[k, 2])
    own_r.wait()
    own_s.wait()
    for c in range(last):
        push(2, c).wait()
    for copy in started:
        copy.wait_send()
    for copy in relays + early:
        pl.when(inner)(copy.wait_send)
    for copy in early:
        pl.when(inner)(copy.wait_recv)
    pl.when(outer)(cross.wait_send)
    pl.when(inner)(cross.wait_recv)
    pl.when(inner)(aside.wait_send)
    pl.when(outer)(aside.wait_recv)


def exchange(left_noise, right_noise, returns, transposed, members, chunks):
    answers, sides = 4, 3
    local, width = right_noise.shape
    cols, tile = transposed.shape
    total = local * members * answers
    count = members * answers
    block = returns.shape[0]
    half = left_noise.dtype
    dma = pltpu.SemaphoreType.DMA
    anywhere = pl.BlockSpec(memory_space=pl.ANY)
    shape = jax.ShapeDtypeStruct
    return pl.pallas_call(
        lambda *refs: exchange_kernel(members, chunks, *refs),
        out_shape=(
            shape((total, tile), half),
            shape((total, width), half),
            shape((count, 1, block), jnp.float32),
            shape((1, block), jnp.float32),
            shape((cols, sum(chunks[:-1])), half),
            shape((cols, chunks[-1]), half),
            shape((cols, chunks[-1]), half),
        ) + tuple(shape((cols, size), half) for _ in range(sides) for size in chunks),
        in_specs=[anywhere] * 4,
        out_specs=(anywhere,) * (7 + sides * len(chunks)),
        scratch_shapes=[
            pltpu.VMEM(left_noise.shape, half), pltpu.VMEM(right_noise.shape, half),
            pltpu.VMEM(returns.shape, returns.dtype), dma((3,)),
            pltpu.VMEM((2, cols, tile // answers), jnp.float32), pltpu.VMEM((2, cols, tile // answers), half),
            pltpu.VMEM((1, block), jnp.float32),
            dma((4,)), dma((sides,)), dma((sides, len(chunks))), dma((4,)), dma((3,)), dma((4,)), dma((4,)),
            dma((1,)), dma((1,)), dma((answers, 2)), dma((answers, 2)),
            dma((4, 2)), dma((3, 2)), dma((4,)), dma((3,)), dma((answers, 3)), dma((answers, 3)),
            dma((len(chunks) - 1,)), dma((len(chunks) - 1,)), dma, dma, dma, dma,
        ],
        compiler_params=pltpu.CompilerParams(collective_id=0, has_side_effects=True),
        name="exchange",
    )(left_noise, right_noise, returns, transposed)


def divisor(size, least, most):
    fits = [n for n in range(least, most + 1, least) if size % n == 0]
    return fits[-1] if fits else size


def final_kernel(picks, where_ref, master_ref, *refs):
    sides, refs = refs[:len(picks)], refs[len(picks):]
    left_ref, right_ref, out_ref, stack = refs[0], refs[1], refs[-2], refs[-1]
    an = lax.axis_index("answer")
    width, rows = master_ref.shape
    near = an + 1 - 2 * lax.rem(an, 2)
    inner = lax.div(an + 1, 2) == 1
    places = {1: near, 2: lax.rem(an + 2, 4), 3: 3 - an}
    within = {True: inner, False: jnp.logical_not(inner)}

    def place(a, ref):
        stack[pl.ds(pl.multiple_of(a * width, 16), width), :] = ref[...].astype(stack.dtype)

    place(an, master_ref)
    for (x, which), ref in zip(picks, sides):
        if which is None:
            place(places[x], ref)
        else:
            pl.when(within[which])(lambda x=x, ref=ref: place(places[x], ref))
    row = lax.broadcasted_iota(jnp.int32, (rows, rows), 0)
    col = lax.broadcasted_iota(jnp.int32, (rows, rows), 1)
    unit = jnp.where(row == col, 1.0, 0.0).astype(stack.dtype)
    step = divisor(out_ref.shape[1], 128, 512)
    for at in range(0, out_ref.shape[1], step):
        cols = slice(at, at + step)
        new = jnp.dot(left_ref[...], right_ref[:, cols], preferred_element_type=jnp.float32)
        old = lax.dot_general(unit, stack[cols, :], (((1,), (1,)), ((), ())), preferred_element_type=jnp.float32)
        out_ref[:, cols] = (new + old).astype(out_ref.dtype)


def finalize(where, transposed, sides, left, right, first, size, so_far):
    rows, members = left.shape
    width = transposed.shape[0]
    total = right.shape[1]
    chunk = 128
    start, steps = first // chunk, size // chunk
    per = rows // chunk
    more = [] if so_far is None else [so_far]
    picks = tuple(key for key, _, _ in sides)
    blocks = [pl.BlockSpec((width, chunk), lambda i, w, at=at: (0, at + i)) for _, _, at in sides]
    return pl.pallas_call(
        lambda *refs: final_kernel(picks, *refs),
        grid_spec=pltpu.PrefetchScalarGridSpec(
            num_scalar_prefetch=1,
            grid=(steps,),
            in_specs=[pl.BlockSpec((width, chunk), lambda i, w: (0, w[0] * per + start + i))] + blocks + [
                pl.BlockSpec((chunk, members), lambda i, w: (start + i, 0)),
                pl.BlockSpec((members, total), lambda i, w: (0, 0)),
            ] + [pl.BlockSpec(memory_space=pl.ANY)] * len(more),
            out_specs=pl.BlockSpec((chunk, total), lambda i, w: (start + i, 0)),
            scratch_shapes=[pltpu.VMEM((total, chunk), jnp.bfloat16)],
        ),
        out_shape=jax.ShapeDtypeStruct((rows, total), jnp.bfloat16),
        input_output_aliases={4 + len(sides): 0} if more else {},
        cost_estimate=pl.CostEstimate(
            flops=2 * size * total * (members + chunk), bytes_accessed=6 * size * total, transcendentals=0),
        compiler_params=pltpu.CompilerParams(vmem_limit_bytes=24 << 20),
        name="final",
    )(where, transposed, *[block for _, block, _ in sides], left, right, *more)


def unit_of(rows, dtype):
    row = lax.broadcasted_iota(jnp.int32, (rows, rows), 0)
    col = lax.broadcasted_iota(jnp.int32, (rows, rows), 1)
    return jnp.where(row == col, 1.0, 0.0).astype(dtype)


def turn(unit, stack):
    return lax.dot_general(unit, stack, (((1,), (1,)), ((), ())), preferred_element_type=jnp.float32)


def lead_kernel(picks, first, master_ref, *refs):
    sides, refs = refs[:len(picks)], refs[len(picks):]
    base_ref, _, out_ref, mix_ref, stack, block, sem = refs
    an = lax.axis_index("answer")
    width, tile = master_ref.shape
    rows = block.shape[0]
    places = {0: an, 1: an + 1 - 2 * lax.rem(an, 2), 2: lax.rem(an + 2, 4), 3: 3 - an}
    inner = lax.div(an + 1, 2) == 1
    within = {True: inner, False: jnp.logical_not(inner)}

    def place(x, value):
        stack[pl.ds(pl.multiple_of(places[x] * width, 16), width), :] = value.astype(stack.dtype)

    stack[...] = jnp.zeros_like(stack)
    place(0, master_ref[:, pl.ds(pl.multiple_of(an * (tile // 4) + first, 128), rows)])
    for (x, which), ref in zip(picks, sides):
        pl.when(within[which])(lambda x=x, ref=ref: place(x, ref[...]))
    unit = unit_of(rows, stack.dtype)
    total = out_ref.shape[1]
    step = divisor(total, 128, 512)
    copies = []
    for i, at in enumerate(range(0, total, step)):
        cols = slice(at, at + step)
        mixed = base_ref[:, cols] + turn(unit, stack[cols, :])
        mix_ref[:, cols] = mixed
        block[:, cols] = mixed.astype(block.dtype)
        copy = pltpu.make_async_copy(block.at[:, cols], out_ref.at[first:first + rows, cols], sem.at[i])
        copy.start()
        copies.append(copy)
    for copy in copies:
        copy.wait()


def lead(transposed, sides, base, first, so_far):
    size, total = base.shape
    vmem, anywhere = pl.BlockSpec(memory_space=pltpu.VMEM), pl.BlockSpec(memory_space=pl.ANY)
    picks = tuple(key for key, _ in sides)
    return pl.pallas_call(
        lambda *refs: lead_kernel(picks, first, *refs),
        in_specs=[vmem] * (2 + len(sides)) + [anywhere],
        out_specs=(anywhere, vmem),
        scratch_shapes=[
            pltpu.VMEM((total, size), so_far.dtype), pltpu.VMEM((size, total), so_far.dtype),
            pltpu.SemaphoreType.DMA((total // divisor(total, 128, 512),)),
        ],
        out_shape=(
            jax.ShapeDtypeStruct(so_far.shape, so_far.dtype),
            jax.ShapeDtypeStruct(base.shape, base.dtype),
        ),
        input_output_aliases={2 + len(sides): 0},
        cost_estimate=pl.CostEstimate(
            flops=2 * size * total * size, bytes_accessed=6 * size * total, transcendentals=0),
        compiler_params=pltpu.CompilerParams(vmem_limit_bytes=24 << 20),
        name="lead",
    )(transposed, *[block for _, block in sides], base, so_far)


def last_kernel(first, mix_ref, inner_ref, outer_ref, _, out_ref, stack, block, sem):
    an = lax.axis_index("answer")
    width, rows = inner_ref.shape
    inner = lax.div(an + 1, 2) == 1
    begin = (2 - lax.div(an, 2)) * width
    low = lax.div(begin, 128) * 128
    at = pl.ds(pl.multiple_of(begin - low, 16), width)
    stack[...] = jnp.zeros_like(stack)

    @pl.when(inner)
    def _():
        stack[at, :] = inner_ref[...]

    @pl.when(jnp.logical_not(inner))
    def _():
        stack[at, :] = outer_ref[...]

    unit = unit_of(rows, stack.dtype)
    step = block.shape[1] // 2
    copies = []
    for i in range(2):
        cols = pl.ds(pl.multiple_of(low + i * step, 128), step)
        mixed = mix_ref[:, cols] + turn(unit, stack[i * step:(i + 1) * step, :])
        block[:, i * step:(i + 1) * step] = mixed.astype(block.dtype)
        copy = pltpu.make_async_copy(
            block.at[:, i * step:(i + 1) * step], out_ref.at[first:first + rows, cols], sem.at[i])
        copy.start()
        copies.append(copy)
    for copy in copies:
        copy.wait()


def finish(mix, inner, outer, first, so_far):
    width, size = inner.shape
    window = -(-(width + 127) // 256) * 256
    vmem, anywhere = pl.BlockSpec(memory_space=pltpu.VMEM), pl.BlockSpec(memory_space=pl.ANY)
    return pl.pallas_call(
        lambda *refs: last_kernel(first, *refs),
        in_specs=[vmem] * 3 + [anywhere],
        out_specs=anywhere,
        scratch_shapes=[
            pltpu.VMEM((window, size), so_far.dtype), pltpu.VMEM((size, window), so_far.dtype),
            pltpu.SemaphoreType.DMA((2,)),
        ],
        out_shape=jax.ShapeDtypeStruct(so_far.shape, so_far.dtype),
        input_output_aliases={3: 0},
        cost_estimate=pl.CostEstimate(
            flops=2 * size * window * size, bytes_accessed=6 * size * window, transcendentals=0),
        compiler_params=pltpu.CompilerParams(vmem_limit_bytes=24 << 20),
        name="last",
    )(mix, inner, outer, so_far)


def update_kernel(master_ref, right_ref, left_ref, new_ref):
    new_ref[...] = master_ref[...] + jnp.dot(right_ref[...], left_ref[...], preferred_element_type=jnp.float32)


def update(transposed, right, left):
    width, tile = transposed.shape
    members = right.shape[1]
    chunk = divisor(width, 16, 150)
    return pl.pallas_call(
        update_kernel,
        grid=(width // chunk,),
        in_specs=[
            pl.BlockSpec((chunk, tile), lambda i: (i, 0)),
            pl.BlockSpec((chunk, members), lambda i: (i, 0)),
            pl.BlockSpec((members, tile), lambda i: (0, 0)),
        ],
        out_specs=pl.BlockSpec((chunk, tile), lambda i: (i, 0)),
        out_shape=jax.ShapeDtypeStruct(transposed.shape, jnp.float32),
        cost_estimate=pl.CostEstimate(
            flops=2 * width * tile * members, bytes_accessed=8 * width * tile, transcendentals=0),
        compiler_params=pltpu.CompilerParams(vmem_limit_bytes=24 << 20),
        name="update",
    )(transposed, right, left)


def weigh_kernel(members, l_ref, r_ref, s_ref, w_ref, o_ref, t_ref, b_ref, turned):
    answers, block = s_ref.shape[0] // members, s_ref.shape[2]
    population = members * block
    local = block // answers
    an = lax.axis_index("answer")
    scores = []
    for m in range(members):
        total = s_ref[m]
        for a in range(1, answers):
            total = total + s_ref[a * members + m]
        scores.append(total)
    average = sum(jnp.sum(x, axis=1, keepdims=True) for x in scores) / population
    squares = sum(jnp.sum(x * x, axis=1, keepdims=True) for x in scores) / population
    spread = jnp.sqrt(squares - average * average + 1e-05) * jnp.sqrt(jnp.float32(population))
    for m in range(members):
        scale = jnp.broadcast_to((scores[m] - average) / spread, (block, block)).T[:, :1]
        for a in range(answers):
            at = (a * members + m) * local
            rows = slice(at, at + local)
            w_ref[rows, :] = (l_ref[rows, :].astype(jnp.float32) * scale[a * local:(a + 1) * local]).astype(w_ref.dtype)
    rows = o_ref.shape[0]
    o_ref[...] = w_ref[:, pl.ds(pl.multiple_of(an * rows, 128), rows)].T
    turned[...] = r_ref[...].T
    width = t_ref.shape[0]
    t_ref[...] = turned[pl.ds(pl.multiple_of(an * width, 16), width), :]
    step = divisor(b_ref.shape[1], 128, 512)
    for at in range(0, b_ref.shape[1], step):
        b_ref[:, at:at + step] = jnp.dot(
            o_ref[rows - b_ref.shape[0]:, :], r_ref[:, at:at + step], preferred_element_type=jnp.float32)


def weigh(left_tile, right, parts, members, rows, width, size):
    vmem = pl.BlockSpec(memory_space=pltpu.VMEM)
    total = left_tile.shape[0]
    half = left_tile.dtype
    return pl.pallas_call(
        lambda *refs: weigh_kernel(members, *refs),
        out_shape=(
            jax.ShapeDtypeStruct(left_tile.shape, half),
            jax.ShapeDtypeStruct((rows, total), half),
            jax.ShapeDtypeStruct((width, total), half),
            jax.ShapeDtypeStruct((size, right.shape[1]), jnp.float32),
        ),
        in_specs=[vmem] * 3,
        out_specs=(vmem,) * 4,
        scratch_shapes=[pltpu.VMEM(right.shape[::-1], half)],
        cost_estimate=pl.CostEstimate(flops=total * right.shape[1] * 256, bytes_accessed=1 << 23, transcendentals=0),
        compiler_params=pltpu.CompilerParams(vmem_limit_bytes=24 << 20),
        name="weigh",
    )(left_tile, right, parts)


def split(rows):
    steps = rows // 128
    last = 1 if steps > 1 else 0
    first = (steps - last + 1) // 2
    return [n * 128 for n in (first, steps - last - first, last) if n]


def order_of(count):
    return [(c, x) for c in range(count) for x in (3, 2, 1)] + [(count - 1, 4)]


def fast_body(master, left_noise, right_noise, returns):
    members, answers = lax.axis_size("member"), lax.axis_size("answer")
    where = lax.axis_index("answer").astype(jnp.int32)[None]
    transposed = master.T
    width, tile = transposed.shape
    rows = tile // answers
    chunks = split(rows)
    last = len(chunks) - 1
    left_tile, right, parts, _, early, cross, aside, *blocks = exchange(left_noise, right_noise, returns, transposed, members, chunks)
    blocks = [blocks[i:i + len(chunks)] for i in range(0, len(blocks), len(chunks))]
    pairs = {1: [(0, 1), (1, 0), (2, 3), (3, 2)], 2: [(1, 3), (2, 0), (0, 2), (3, 1)], 3: [(0, 3), (3, 0)], 4: [(1, 2), (2, 1)]}
    got = {}
    for c, x in order_of(len(chunks)):
        some = {(last, 2): pairs[2][:2], (last, 1): pairs[1][::3]}.get((c, x), pairs[x])
        got[c, x] = lax.ppermute(blocks[min(x, 3) - 1][c], "answer", some)
    weighted, own, turned, base = weigh(left_tile, right, parts, members, rows, width, chunks[-1])
    new_master = update(transposed, turned, weighted)
    rollout, at = None, 0
    for c, size in enumerate(chunks):
        if c == last:
            sides = [((1, True), got[c, 1]), ((1, False), aside), ((2, True), cross), ((3, False), got[c, 3])]
            rollout, mix = lead(transposed, sides, base, at, rollout)
            rollout = finish(mix, got[c, 4], got[c, 2], at, rollout)
        else:
            sides = [((1, None), got[c, 1], 0), ((2, None), got[c, 2], 0),
                     ((3, False), got[c, 3], 0), ((3, True), early, at // 128)]
            rollout = finalize(where, transposed, sides, own, right, at, size, rollout)
        at += size
    return (new_master.T, rollout)


def fits(members, tensors, answers, tile, width, local):
    return (members, tensors, answers) == (2, 4, 4) and tile % 512 == 0 and tile >= 1024 and width >= 512 and local % 32 == 0


def body(master, left_noise, right_noise, returns):
    sizes = [lax.axis_size(n) for n in ("member", "tensor", "answer")]
    fast = fits(*sizes, *master.shape, left_noise.shape[0])
    return (fast_body if fast else plain_body)(master, left_noise, right_noise, returns)


def solution(mesh):
    return jax.shard_map(
        body,
        mesh=mesh,
        in_specs=(
            P("member", ("tensor", "answer")),
            P(("member", "answer"), None),
            P(("member", "answer"), "tensor"),
            P("member", "answer"),
        ),
        out_specs=(P("member", ("tensor", "answer")), P(("member", "answer"), "tensor")),
        check_vma=False,
    )
```

```python
import jax
import jax.numpy as jnp
from jax import lax
from jax.experimental import pallas as pl
from jax.experimental.pallas import tpu as pltpu
from jax.sharding import PartitionSpec as P


def contract(left_tile, accum, pieces):
    right_cols, weights = pieces
    weighted = left_tile.astype(jnp.float32) * weights[:, None]
    return accum + lax.dot_general(
        weighted,
        right_cols.astype(jnp.float32),
        (((0,), (0,)), ((), ())),
        precision=lax.Precision.HIGHEST,
    )


def plain_body(master, left_noise, right_noise, returns):
    member_count = lax.axis_size("member")
    answer_count = lax.axis_size("answer")
    partial_value = jnp.sum(returns, axis=1)
    block_len = partial_value.shape[0]
    population = block_len * member_count
    scores = lax.psum(partial_value, "answer")
    score_sum, square_sum = lax.psum((jnp.sum(scores), jnp.sum(scores * scores)), "member")
    average = score_sum / population
    variance = square_sum / population - average * average
    fitness = (scores - average) / jnp.sqrt(variance + 1e-05)
    tile_rows = master.shape[0]
    local_members = left_noise.shape[0]
    restricted = lax.all_to_all(left_noise, "member", split_axis=1, concat_axis=0, tiled=True)
    gathered_rows = lax.all_gather(restricted, "answer", axis=0, tiled=True)
    width = gathered_rows.shape[1]
    left_tile = gathered_rows.reshape(answer_count, member_count, local_members, width)
    left_tile = jnp.transpose(left_tile, (1, 0, 2, 3)).reshape(
        answer_count * member_count * local_members, width
    )
    right_block = lax.all_to_all(right_noise, "answer", split_axis=1, concat_axis=0, tiled=True)
    initial = jnp.zeros((tile_rows, right_block.shape[1]), jnp.float32)
    update = contract(
        left_tile,
        initial,
        (
            lax.all_gather(right_block, "member", axis=0, tiled=True),
            lax.all_gather(fitness.astype(jnp.bfloat16), "member", axis=0, tiled=True).astype(
                jnp.float32
            ),
        ),
    )
    new_master = master + update / jnp.sqrt(jnp.float32(population))
    rollout = lax.all_to_all(
        new_master.astype(jnp.bfloat16), "answer", split_axis=0, concat_axis=1, tiled=True
    )
    return (new_master, rollout)


def exchange_kernel(members, chunks, left_hbm, right_hbm, returns_hbm, master_ref, *refs):
    sides = 3
    l_ref, r_ref, s_ref, p_ref, e_ref, n_ref, b_ref, *refs = refs
    blocks, refs = refs[:sides * len(chunks)], refs[sides * len(chunks):]
    (left_ref, right_ref, returns_ref, load_sem, wide, narrow, part, own_sem, pull_sem, push_sem, s_send, s_recv, t_send, t_recv, x_send, x_recv, f_send, f_recv,
     z_send, z_recv, q_send, q_recv, y_send, y_recv, e_send, e_recv, n_send, n_recv, b_send, b_recv) = refs
    me, te, an = lax.axis_index("member"), lax.axis_index("tensor"), lax.axis_index("answer")
    answers = 4
    local = left_ref.shape[0]
    slab = local * members
    tile = l_ref.shape[1]
    piece = tile // 4
    rows = tile // answers
    beside = lambda i: i + 1 - 2 * lax.rem(i, 2)
    other, core, across = 1 - me, beside(te), lax.rem(te + 2, 4)
    near, far = beside(an), 2 - lax.div(an, 2)
    beyond = 2 * (1 - lax.div(an, 2))
    inner = lax.div(an + 1, 2) == 1
    outer = jnp.logical_not(inner)
    pair = {1: near, 2: lax.rem(an + 2, answers), 3: answers - 1 - an}

    def l_at(start, count, t):
        return l_ref.at[pl.ds(pl.multiple_of(start, local), count), pl.ds(pl.multiple_of(t * piece, piece), piece)]

    def l_slab(a, t):
        return l_at(a * slab, slab, t)

    def r_at(a, m):
        return r_ref.at[pl.ds(pl.multiple_of((a * members + m) * local, local), local), :]

    def remote(src, dst, send, recv, where):
        return pltpu.make_async_remote_copy(src_ref=src, dst_ref=dst, send_sem=send, recv_sem=recv,
                                            device_id=where, device_id_type=pl.DeviceIdType.MESH)

    def pull(x):
        return pltpu.make_async_copy(
            master_ref.at[:, pl.ds(pl.multiple_of(pair[x] * rows, rows), rows)], wide.at[x % 2], pull_sem.at[x - 1])

    def push(x, c):
        at = sum(chunks[:c])
        return pltpu.make_async_copy(
            narrow.at[x % 2, :, at:at + chunks[c]], blocks[(x - 1) * len(chunks) + c], push_sem.at[x - 1, c])

    def cast(x):
        pull(x).wait()
        step = 96

        def one(i, _):
            at = pl.ds(pl.multiple_of(i * step, step), step)
            narrow[x % 2, at, :] = wide[x % 2, at, :].astype(narrow.dtype)
            return 0

        lax.fori_loop(0, narrow.shape[1] // step, one, 0)
        for c in range(len(chunks)):
            push(x, c).start()

    barrier = pltpu.get_barrier_semaphore()

    def greet(where):
        pl.semaphore_signal(barrier, inc=1, device_id=where, device_id_type=pl.DeviceIdType.MESH)

    for where in ({"answer": near}, {"member": other}, {"tensor": core}, {"tensor": across}):
        greet(where)

    @pl.when(inner)
    def _():
        greet({"answer": beyond})
        greet({"answer": beyond + 1})

    loads = [pltpu.make_async_copy(src, dst, load_sem.at[i]) for i, (src, dst) in enumerate(
        ((right_hbm, right_ref), (left_hbm, left_ref), (returns_hbm, returns_ref)))]
    for load in loads:
        load.start()
    pull(1).start()
    pull(2).start()
    loads[0].wait()
    own_r = pltpu.make_async_copy(right_ref, r_at(an, me), own_sem.at[1])
    own_r.start()
    pl.semaphore_wait(barrier, 5)

    mine = lax.rem(an, 2)
    halves = 4
    count = local // halves
    sources = (an, near, beyond, beyond + 1)
    started = []

    def start(copy):
        copy.start()
        started.append(copy)
        return copy

    def landed(block, sem):
        remote(block, block, x_send.at[0], sem, {"member": other}).wait_recv()

    def r_half(a, m, h):
        return r_ref.at[pl.ds(pl.multiple_of((a * members + m) * local + h * count, count), count), :]

    def forward(k, h):
        block = r_half(sources[k], me, h)
        src = right_ref.at[h * count:(h + 1) * count, :] if k == 0 else block
        start(remote(src, block, f_send.at[k, h], f_recv.at[k, h], {"member": other}))

    def spread(k):
        block = l_slab(sources[k], te)
        start(remote(block, block, y_send.at[k, 0], y_recv.at[k, 0], {"tensor": across}))
        start(remote(block, block, y_send.at[k, 1], y_recv.at[k, 1], {"tensor": core}))

    def part_of(h):
        src = right_ref.at[h * count:(h + 1) * count, :]
        start(remote(src, r_half(an, me, h), z_send.at[0, h], z_recv.at[1 + mine, h], {"answer": far}))
        start(remote(src, r_half(an, me, h), z_send.at[1, h], z_recv.at[0, h], {"answer": near}))

    part_of(0)
    loads[1].wait()
    start(remote(left_ref.at[:, pl.ds(pl.multiple_of(other * tile + te * piece, piece), piece)],
                 l_at((an * members + me) * local, local, te), x_send.at[0], x_recv.at[0], {"member": other}))
    own_l = pltpu.make_async_copy(
        left_ref.at[:, pl.ds(pl.multiple_of(me * tile + te * piece, piece), piece)],
        l_at((an * members + me) * local, local, te), own_sem.at[0])
    own_l.start()
    loads[2].wait()
    part[...] = jnp.sum(returns_ref[...].T, axis=0, keepdims=True)
    own_p = pltpu.make_async_copy(part, p_ref, own_sem.at[2])
    own_s = pltpu.make_async_copy(part, s_ref.at[an * members + me], own_sem.at[3])
    own_p.start()
    own_s.start()
    own_p.wait()
    score = lambda a, m: s_ref.at[a * members + m]
    start(remote(p_ref, score(an, me), s_send.at[0], s_recv.at[mine + 1], {"answer": far}))
    start(remote(p_ref, score(an, me), s_send.at[1], s_recv.at[0], {"answer": near}))
    start(remote(p_ref, score(an, me), t_send.at[0], t_recv.at[0], {"member": other}))
    own_l.wait()
    landed(l_at((an * members + other) * local, local, te), x_recv.at[0])
    block = l_slab(an, te)
    start(remote(block, block, q_send.at[0], q_recv.at[1 + mine], {"answer": far}))
    start(remote(block, block, q_send.at[1], q_recv.at[0], {"answer": near}))
    for h in range(1, halves):
        part_of(h)
    spread(0)
    for h in range(halves):
        forward(0, h)
    last = len(chunks) - 1
    cast(1)
    push(1, last).wait()
    aside = remote(blocks[last], b_ref, b_send, b_recv, {"answer": near})
    pl.when(inner)(aside.start)
    for c in range(last):
        push(1, c).wait()
    pull(3).start()
    cast(2)
    push(2, last).wait()
    cross = remote(blocks[len(chunks) + last], n_ref, n_send, n_recv, {"answer": far})
    pl.when(outer)(cross.start)
    cast(3)
    early = []
    push(3, last).wait()
    for c, size in enumerate(chunks[:last]):
        push(3, c).wait()
        at = sum(chunks[:c])
        copy = remote(blocks[2 * len(chunks) + c], e_ref.at[:, at:at + size], e_send.at[c], e_recv.at[c], {"answer": pair[3]})
        pl.when(inner)(copy.start)
        early.append(copy)
    for h in range(halves):
        landed(r_half(near, me, h), z_recv.at[0, h])
        forward(1, h)
    landed(l_slab(near, te), q_recv.at[0])
    spread(1)
    relays = []

    def relay(block, send, recv):
        copy = remote(block, block, send, recv, {"answer": near})
        pl.when(inner)(copy.start)
        relays.append(copy)

    def pass_on(h):
        for k in (2, 3):
            block = r_half(sources[k], me, h)
            landed(block, z_recv.at[k - 1, h])
            relay(block, z_send.at[k, h], z_recv.at[k - 1, h])
            forward(k, h)

    pass_on(0)
    for k in (2, 3):
        block = l_slab(sources[k], te)
        landed(block, q_recv.at[k - 1])
        relay(block, q_send.at[k], q_recv.at[k - 1])
        spread(k)
    for h in range(1, halves):
        pass_on(h)
    for k in range(answers):
        block = l_slab(sources[k], across)
        landed(block, y_recv.at[k, 0])
        start(remote(block, block, y_send.at[k, 2], y_recv.at[k, 2], {"tensor": core}))
    for k in range(1, answers):
        block = score(sources[k], me)
        landed(block, s_recv.at[k - 1])
        if k > 1:
            relay(block, s_send.at[k], s_recv.at[k - 1])
        start(remote(block, block, t_send.at[k], t_recv.at[k], {"member": other}))
    for k in range(answers):
        landed(score(sources[k], other), t_recv.at[k])
    for k in range(answers):
        for h in range(halves):
            landed(r_half(sources[k], other, h), f_recv.at[k, h])
    for k in range(answers):
        landed(l_slab(sources[k], core), y_recv.at[k, 1])
        landed(l_slab(sources[k], 3 - te), y_recv.at[k, 2])
    own_r.wait()
    own_s.wait()
    for c in range(last):
        push(2, c).wait()
    for copy in started:
        copy.wait_send()
    for copy in relays + early:
        pl.when(inner)(copy.wait_send)
    for copy in early:
        pl.when(inner)(copy.wait_recv)
    pl.when(outer)(cross.wait_send)
    pl.when(inner)(cross.wait_recv)
    pl.when(inner)(aside.wait_send)
    pl.when(outer)(aside.wait_recv)


def exchange(left_noise, right_noise, returns, transposed, members, chunks):
    answers, sides = 4, 3
    local, width = right_noise.shape
    cols, tile = transposed.shape
    total = local * members * answers
    count = members * answers
    block = returns.shape[0]
    half = left_noise.dtype
    dma = pltpu.SemaphoreType.DMA
    anywhere = pl.BlockSpec(memory_space=pl.ANY)
    shape = jax.ShapeDtypeStruct
    return pl.pallas_call(
        lambda *refs: exchange_kernel(members, chunks, *refs),
        out_shape=(
            shape((total, tile), half),
            shape((total, width), half),
            shape((count, 1, block), jnp.float32),
            shape((1, block), jnp.float32),
            shape((cols, sum(chunks[:-1])), half),
            shape((cols, chunks[-1]), half),
            shape((cols, chunks[-1]), half),
        ) + tuple(shape((cols, size), half) for _ in range(sides) for size in chunks),
        in_specs=[anywhere] * 4,
        out_specs=(anywhere,) * (7 + sides * len(chunks)),
        scratch_shapes=[
            pltpu.VMEM(left_noise.shape, half), pltpu.VMEM(right_noise.shape, half),
            pltpu.VMEM(returns.shape, returns.dtype), dma((3,)),
            pltpu.VMEM((2, cols, tile // answers), jnp.float32), pltpu.VMEM((2, cols, tile // answers), half),
            pltpu.VMEM((1, block), jnp.float32),
            dma((4,)), dma((sides,)), dma((sides, len(chunks))), dma((4,)), dma((3,)), dma((4,)), dma((4,)),
            dma((1,)), dma((1,)), dma((answers, 4)), dma((answers, 4)),
            dma((4, 4)), dma((3, 4)), dma((4,)), dma((3,)), dma((answers, 3)), dma((answers, 3)),
            dma((len(chunks) - 1,)), dma((len(chunks) - 1,)), dma, dma, dma, dma,
        ],
        compiler_params=pltpu.CompilerParams(collective_id=0, has_side_effects=True),
        name="exchange",
    )(left_noise, right_noise, returns, transposed)


def divisor(size, least, most):
    fits = [n for n in range(least, most + 1, least) if size % n == 0]
    return fits[-1] if fits else size


def final_kernel(picks, where_ref, master_ref, *refs):
    sides, refs = refs[:len(picks)], refs[len(picks):]
    left_ref, right_ref, out_ref, stack = refs[0], refs[1], refs[-2], refs[-1]
    an = lax.axis_index("answer")
    width, rows = master_ref.shape
    near = an + 1 - 2 * lax.rem(an, 2)
    inner = lax.div(an + 1, 2) == 1
    places = {1: near, 2: lax.rem(an + 2, 4), 3: 3 - an}
    within = {True: inner, False: jnp.logical_not(inner)}

    def place(a, ref):
        stack[pl.ds(pl.multiple_of(a * width, 16), width), :] = ref[...].astype(stack.dtype)

    place(an, master_ref)
    for (x, which), ref in zip(picks, sides):
        if which is None:
            place(places[x], ref)
        else:
            pl.when(within[which])(lambda x=x, ref=ref: place(places[x], ref))
    row = lax.broadcasted_iota(jnp.int32, (rows, rows), 0)
    col = lax.broadcasted_iota(jnp.int32, (rows, rows), 1)
    unit = jnp.where(row == col, 1.0, 0.0).astype(stack.dtype)
    step = divisor(out_ref.shape[1], 128, 512)
    for at in range(0, out_ref.shape[1], step):
        cols = slice(at, at + step)
        new = jnp.dot(left_ref[...], right_ref[:, cols], preferred_element_type=jnp.float32)
        old = lax.dot_general(unit, stack[cols, :], (((1,), (1,)), ((), ())), preferred_element_type=jnp.float32)
        out_ref[:, cols] = (new + old).astype(out_ref.dtype)


def finalize(where, transposed, sides, left, right, first, size, so_far):
    rows, members = left.shape
    width = transposed.shape[0]
    total = right.shape[1]
    chunk = 128
    start, steps = first // chunk, size // chunk
    per = rows // chunk
    more = [] if so_far is None else [so_far]
    picks = tuple(key for key, _, _ in sides)
    blocks = [pl.BlockSpec((width, chunk), lambda i, w, at=at: (0, at + i)) for _, _, at in sides]
    return pl.pallas_call(
        lambda *refs: final_kernel(picks, *refs),
        grid_spec=pltpu.PrefetchScalarGridSpec(
            num_scalar_prefetch=1,
            grid=(steps,),
            in_specs=[pl.BlockSpec((width, chunk), lambda i, w: (0, w[0] * per + start + i))] + blocks + [
                pl.BlockSpec((chunk, members), lambda i, w: (start + i, 0)),
                pl.BlockSpec((members, total), lambda i, w: (0, 0)),
            ] + [pl.BlockSpec(memory_space=pl.ANY)] * len(more),
            out_specs=pl.BlockSpec((chunk, total), lambda i, w: (start + i, 0)),
            scratch_shapes=[pltpu.VMEM((total, chunk), jnp.bfloat16)],
        ),
        out_shape=jax.ShapeDtypeStruct((rows, total), jnp.bfloat16),
        input_output_aliases={4 + len(sides): 0} if more else {},
        cost_estimate=pl.CostEstimate(
            flops=2 * size * total * (members + chunk), bytes_accessed=6 * size * total, transcendentals=0),
        compiler_params=pltpu.CompilerParams(vmem_limit_bytes=24 << 20),
        name="final",
    )(where, transposed, *[block for _, block, _ in sides], left, right, *more)


def unit_of(rows, dtype):
    row = lax.broadcasted_iota(jnp.int32, (rows, rows), 0)
    col = lax.broadcasted_iota(jnp.int32, (rows, rows), 1)
    return jnp.where(row == col, 1.0, 0.0).astype(dtype)


def turn(unit, stack):
    return lax.dot_general(unit, stack, (((1,), (1,)), ((), ())), preferred_element_type=jnp.float32)


def lead_kernel(picks, first, master_ref, *refs):
    sides, refs = refs[:len(picks)], refs[len(picks):]
    base_ref, _, out_ref, mix_ref, stack, block, sem = refs
    an = lax.axis_index("answer")
    width, tile = master_ref.shape
    rows = block.shape[0]
    places = {0: an, 1: an + 1 - 2 * lax.rem(an, 2), 2: lax.rem(an + 2, 4), 3: 3 - an}
    inner = lax.div(an + 1, 2) == 1
    within = {True: inner, False: jnp.logical_not(inner)}

    def place(x, value):
        stack[pl.ds(pl.multiple_of(places[x] * width, 16), width), :] = value.astype(stack.dtype)

    stack[...] = jnp.zeros_like(stack)
    place(0, master_ref[:, pl.ds(pl.multiple_of(an * (tile // 4) + first, 128), rows)])
    for (x, which), ref in zip(picks, sides):
        pl.when(within[which])(lambda x=x, ref=ref: place(x, ref[...]))
    unit = unit_of(rows, stack.dtype)
    total = out_ref.shape[1]
    step = divisor(total, 128, 512)
    copies = []
    for i, at in enumerate(range(0, total, step)):
        cols = slice(at, at + step)
        mixed = base_ref[:, cols] + turn(unit, stack[cols, :])
        mix_ref[:, cols] = mixed
        block[:, cols] = mixed.astype(block.dtype)
        copy = pltpu.make_async_copy(block.at[:, cols], out_ref.at[first:first + rows, cols], sem.at[i])
        copy.start()
        copies.append(copy)
    for copy in copies:
        copy.wait()


def lead(transposed, sides, base, first, so_far):
    size, total = base.shape
    vmem, anywhere = pl.BlockSpec(memory_space=pltpu.VMEM), pl.BlockSpec(memory_space=pl.ANY)
    picks = tuple(key for key, _ in sides)
    return pl.pallas_call(
        lambda *refs: lead_kernel(picks, first, *refs),
        in_specs=[vmem] * (2 + len(sides)) + [anywhere],
        out_specs=(anywhere, vmem),
        scratch_shapes=[
            pltpu.VMEM((total, size), so_far.dtype), pltpu.VMEM((size, total), so_far.dtype),
            pltpu.SemaphoreType.DMA((total // divisor(total, 128, 512),)),
        ],
        out_shape=(
            jax.ShapeDtypeStruct(so_far.shape, so_far.dtype),
            jax.ShapeDtypeStruct(base.shape, base.dtype),
        ),
        input_output_aliases={2 + len(sides): 0},
        cost_estimate=pl.CostEstimate(
            flops=2 * size * total * size, bytes_accessed=6 * size * total, transcendentals=0),
        compiler_params=pltpu.CompilerParams(vmem_limit_bytes=24 << 20),
        name="lead",
    )(transposed, *[block for _, block in sides], base, so_far)


def last_kernel(first, mix_ref, inner_ref, outer_ref, _, out_ref, stack, block, sem):
    an = lax.axis_index("answer")
    width, rows = inner_ref.shape
    inner = lax.div(an + 1, 2) == 1
    begin = (2 - lax.div(an, 2)) * width
    low = lax.div(begin, 128) * 128
    at = pl.ds(pl.multiple_of(begin - low, 16), width)
    stack[...] = jnp.zeros_like(stack)

    @pl.when(inner)
    def _():
        stack[at, :] = inner_ref[...]

    @pl.when(jnp.logical_not(inner))
    def _():
        stack[at, :] = outer_ref[...]

    unit = unit_of(rows, stack.dtype)
    step = block.shape[1] // 2
    copies = []
    for i in range(2):
        cols = pl.ds(pl.multiple_of(low + i * step, 128), step)
        mixed = mix_ref[:, cols] + turn(unit, stack[i * step:(i + 1) * step, :])
        block[:, i * step:(i + 1) * step] = mixed.astype(block.dtype)
        copy = pltpu.make_async_copy(
            block.at[:, i * step:(i + 1) * step], out_ref.at[first:first + rows, cols], sem.at[i])
        copy.start()
        copies.append(copy)
    for copy in copies:
        copy.wait()


def finish(mix, inner, outer, first, so_far):
    width, size = inner.shape
    window = -(-(width + 127) // 256) * 256
    vmem, anywhere = pl.BlockSpec(memory_space=pltpu.VMEM), pl.BlockSpec(memory_space=pl.ANY)
    return pl.pallas_call(
        lambda *refs: last_kernel(first, *refs),
        in_specs=[vmem] * 3 + [anywhere],
        out_specs=anywhere,
        scratch_shapes=[
            pltpu.VMEM((window, size), so_far.dtype), pltpu.VMEM((size, window), so_far.dtype),
            pltpu.SemaphoreType.DMA((2,)),
        ],
        out_shape=jax.ShapeDtypeStruct(so_far.shape, so_far.dtype),
        input_output_aliases={3: 0},
        cost_estimate=pl.CostEstimate(
            flops=2 * size * window * size, bytes_accessed=6 * size * window, transcendentals=0),
        compiler_params=pltpu.CompilerParams(vmem_limit_bytes=24 << 20),
        name="last",
    )(mix, inner, outer, so_far)


def update_kernel(master_ref, right_ref, left_ref, new_ref):
    new_ref[...] = master_ref[...] + jnp.dot(right_ref[...], left_ref[...], preferred_element_type=jnp.float32)


def update(transposed, right, left):
    width, tile = transposed.shape
    members = right.shape[1]
    chunk = divisor(width, 16, 150)
    return pl.pallas_call(
        update_kernel,
        grid=(width // chunk,),
        in_specs=[
            pl.BlockSpec((chunk, tile), lambda i: (i, 0)),
            pl.BlockSpec((chunk, members), lambda i: (i, 0)),
            pl.BlockSpec((members, tile), lambda i: (0, 0)),
        ],
        out_specs=pl.BlockSpec((chunk, tile), lambda i: (i, 0)),
        out_shape=jax.ShapeDtypeStruct(transposed.shape, jnp.float32),
        cost_estimate=pl.CostEstimate(
            flops=2 * width * tile * members, bytes_accessed=8 * width * tile, transcendentals=0),
        compiler_params=pltpu.CompilerParams(vmem_limit_bytes=24 << 20),
        name="update",
    )(transposed, right, left)


def weigh_kernel(members, l_ref, r_ref, s_ref, w_ref, o_ref, t_ref, b_ref, turned):
    answers, block = s_ref.shape[0] // members, s_ref.shape[2]
    population = members * block
    local = block // answers
    an = lax.axis_index("answer")
    scores = []
    for m in range(members):
        total = s_ref[m]
        for a in range(1, answers):
            total = total + s_ref[a * members + m]
        scores.append(total)
    average = sum(jnp.sum(x, axis=1, keepdims=True) for x in scores) / population
    squares = sum(jnp.sum(x * x, axis=1, keepdims=True) for x in scores) / population
    spread = jnp.sqrt(squares - average * average + 1e-05) * jnp.sqrt(jnp.float32(population))
    for m in range(members):
        scale = jnp.broadcast_to((scores[m] - average) / spread, (block, block)).T[:, :1]
        for a in range(answers):
            at = (a * members + m) * local
            rows = slice(at, at + local)
            w_ref[rows, :] = (l_ref[rows, :].astype(jnp.float32) * scale[a * local:(a + 1) * local]).astype(w_ref.dtype)
    rows = o_ref.shape[0]
    o_ref[...] = w_ref[:, pl.ds(pl.multiple_of(an * rows, 128), rows)].T
    turned[...] = r_ref[...].T
    width = t_ref.shape[0]
    t_ref[...] = turned[pl.ds(pl.multiple_of(an * width, 16), width), :]
    step = divisor(b_ref.shape[1], 128, 512)
    for at in range(0, b_ref.shape[1], step):
        b_ref[:, at:at + step] = jnp.dot(
            o_ref[rows - b_ref.shape[0]:, :], r_ref[:, at:at + step], preferred_element_type=jnp.float32)


def weigh(left_tile, right, parts, members, rows, width, size):
    vmem = pl.BlockSpec(memory_space=pltpu.VMEM)
    total = left_tile.shape[0]
    half = left_tile.dtype
    return pl.pallas_call(
        lambda *refs: weigh_kernel(members, *refs),
        out_shape=(
            jax.ShapeDtypeStruct(left_tile.shape, half),
            jax.ShapeDtypeStruct((rows, total), half),
            jax.ShapeDtypeStruct((width, total), half),
            jax.ShapeDtypeStruct((size, right.shape[1]), jnp.float32),
        ),
        in_specs=[vmem] * 3,
        out_specs=(vmem,) * 4,
        scratch_shapes=[pltpu.VMEM(right.shape[::-1], half)],
        cost_estimate=pl.CostEstimate(flops=total * right.shape[1] * 256, bytes_accessed=1 << 23, transcendentals=0),
        compiler_params=pltpu.CompilerParams(vmem_limit_bytes=24 << 20),
        name="weigh",
    )(left_tile, right, parts)


def split(rows):
    steps = rows // 128
    last = 1 if steps > 1 else 0
    first = (steps - last + 1) // 2
    return [n * 128 for n in (first, steps - last - first, last) if n]


def order_of(count):
    return [(c, x) for c in range(count) for x in (3, 2, 1)] + [(count - 1, 4)]


def fast_body(master, left_noise, right_noise, returns):
    members, answers = lax.axis_size("member"), lax.axis_size("answer")
    where = lax.axis_index("answer").astype(jnp.int32)[None]
    transposed = master.T
    width, tile = transposed.shape
    rows = tile // answers
    chunks = split(rows)
    last = len(chunks) - 1
    left_tile, right, parts, _, early, cross, aside, *blocks = exchange(left_noise, right_noise, returns, transposed, members, chunks)
    blocks = [blocks[i:i + len(chunks)] for i in range(0, len(blocks), len(chunks))]
    pairs = {1: [(0, 1), (1, 0), (2, 3), (3, 2)], 2: [(1, 3), (2, 0), (0, 2), (3, 1)], 3: [(0, 3), (3, 0)], 4: [(1, 2), (2, 1)]}
    got = {}
    for c, x in order_of(len(chunks)):
        some = {(last, 2): pairs[2][:2], (last, 1): pairs[1][::3]}.get((c, x), pairs[x])
        got[c, x] = lax.ppermute(blocks[min(x, 3) - 1][c], "answer", some)
    weighted, own, turned, base = weigh(left_tile, right, parts, members, rows, width, chunks[-1])
    new_master = update(transposed, turned, weighted)
    rollout, starts = None, [sum(chunks[:c]) for c in range(len(chunks))]
    sides = [((1, True), got[last, 1]), ((1, False), aside), ((2, True), cross), ((3, False), got[last, 3])]
    for c in range(last):
        picks = [((1, None), got[c, 1], 0), ((2, None), got[c, 2], 0),
                 ((3, False), got[c, 3], 0), ((3, True), early, starts[c] // 128)]
        rollout = finalize(where, transposed, picks, own, right, starts[c], chunks[c], rollout)
        if c == 0:
            rollout, mix = lead(transposed, sides, base, starts[last], rollout)
    rollout = finish(mix, got[last, 4], got[last, 2], starts[last], rollout)
    return (new_master.T, rollout)


def fits(members, tensors, answers, tile, width, local):
    return (members, tensors, answers) == (2, 4, 4) and tile % 512 == 0 and tile >= 1024 and width >= 512 and local % 32 == 0


def body(master, left_noise, right_noise, returns):
    sizes = [lax.axis_size(n) for n in ("member", "tensor", "answer")]
    fast = fits(*sizes, *master.shape, left_noise.shape[0])
    return (fast_body if fast else plain_body)(master, left_noise, right_noise, returns)


def solution(mesh):
    return jax.shard_map(
        body,
        mesh=mesh,
        in_specs=(
            P("member", ("tensor", "answer")),
            P(("member", "answer"), None),
            P(("member", "answer"), "tensor"),
            P("member", "answer"),
        ),
        out_specs=(P("member", ("tensor", "answer")), P(("member", "answer"), "tensor")),
        check_vma=False,
    )
```
